32 devices in a mesh: row: 4 (over x, core), theta: 4 (over z), phi: 2 (over y).
Axes of the slice: x: 2, y: 2, z: 4, core: 2. Of those that a mesh axis runs over, the one named last changes fastest.
Arguments:
- magnetic: float32 [3, 48, 64, 256], P(None, 'row', 'theta', 'phi'), may hold values from -6 to 6
- electric: float32 [3, 48, 64, 256], P(None, 'row', 'theta', 'phi'), may hold values from -6 to 6
Outputs:
- magnetic_new: float32 [3, 48, 64, 256], P(None, 'row', 'theta', 'phi')
- electric_new: float32 [3, 48, 64, 256], P(None, 'row', 'theta', 'phi')
The draws below stay inside these ranges and needn't reach their ends.
All inputs are finite; a program needn't handle non-finite values.
Results may differ from the reference program's by a relative error of at most 0.0001.
Values sent between devices are 32-bit elements; how exact they have to be, the bound alone decides.
A program may use at most 64 MiB of HBM per device.

```python
import math
import jax
import jax.numpy as jnp
from jax import lax

NR = 48
NT = 64
NP = 256


def steps_of(rng, dims, pieces, smallest, high):
    def one(dim, shards_of):
        steps = jax.random.uniform(jax.random.fold_in(jax.random.fold_in(rng, 6), dim), (shards_of,), jnp.float32, smallest / len(pieces), high / len(pieces))
        return jnp.repeat(jnp.exp(steps), dims[dim] // shards_of).reshape((-1,) + (1,) * (len(dims) - dim - 1))

    loudness = one(*pieces[0])
    for cut in pieces[1:]:
        loudness = loudness * one(*cut)
    return loudness


def gaussian(own_key, extent, width, most, shards=(), kind=jnp.bfloat16):
    result = width * jax.random.normal(own_key, extent, jnp.float32)
    if shards:
        result = result * steps_of(own_key, extent, shards, -0.22, 0.18)
    return jnp.clip(result, -most, most).astype(kind)


def setup_inputs(seed: int = 0) -> dict:
    key_of = jax.random.split(jax.random.key(seed), 3)
    return {
        "magnetic": gaussian(key_of[0], (3, NR, NT, NP), 1.0, 6.0, ((1, 4), (2, 4), (3, 2)), jnp.float32),
        "electric": gaussian(key_of[1], (3, NR, NT, NP), 1.0, 6.0, ((1, 4), (2, 4), (3, 2)), jnp.float32),
    }


hole_mass = 1.0
inner_radius = 1.8
wave_speed = 1.25
courant = 0.3
smooth_eps = 1e-06

def weno_face(far_left, near_left, center, near_right, far_right):
    cand_low = (2.0 * far_left - 7.0 * near_left + 11.0 * center) / 6.0
    cand_mid = (-near_left + 5.0 * center + 2.0 * near_right) / 6.0
    cand_high = (2.0 * center + 5.0 * near_right - far_right) / 6.0
    rough_low = 13.0 / 12.0 * (far_left - 2.0 * near_left + center) ** 2 + 0.25 * (far_left - 4.0 * near_left + 3.0 * center) ** 2
    rough_mid = 13.0 / 12.0 * (near_left - 2.0 * center + near_right) ** 2 + 0.25 * (near_left - near_right) ** 2
    rough_high = 13.0 / 12.0 * (center - 2.0 * near_right + far_right) ** 2 + 0.25 * (3.0 * center - 4.0 * near_right + far_right) ** 2
    alpha_low = 0.1 / (smooth_eps + rough_low) ** 2
    alpha_mid = 0.6 / (smooth_eps + rough_mid) ** 2
    alpha_high = 0.3 / (smooth_eps + rough_high) ** 2
    return (alpha_low * cand_low + alpha_mid * cand_mid + alpha_high * cand_high) / (alpha_low + alpha_mid + alpha_high)

def interface(flux, field, axis):
    faces = flux.shape[axis] - 5
    plus_part = 0.5 * (flux + wave_speed * field)
    minus_part = 0.5 * (flux - wave_speed * field)
    plus_cuts = [lax.slice_in_dim(plus_part, offset, offset + faces, axis=axis) for offset in range(6)]
    minus_cuts = [lax.slice_in_dim(minus_part, offset, offset + faces, axis=axis) for offset in range(6)]
    left_state = weno_face(plus_cuts[0], plus_cuts[1], plus_cuts[2], plus_cuts[3], plus_cuts[4])
    right_state = weno_face(minus_cuts[5], minus_cuts[4], minus_cuts[3], minus_cuts[2], minus_cuts[1])
    return left_state + right_state

def face_fluxes(fluxes, fields, axis):
    return lax.map(lambda couple: interface(couple[0], couple[1], axis), (fluxes, fields))

def tendency(padded, radii, angles, spacing_r, spacing_theta, spacing_phi):
    ratio = 2.0 * hole_mass / radii
    lapse_factor = (1.0 / jnp.sqrt(1.0 + ratio))[:, None, None]
    shift_speed = (ratio / (1.0 + ratio))[:, None, None]
    b_radial, b_polar, b_azimuth = (padded[0], padded[1], padded[2])
    d_radial, d_polar, d_azimuth = (padded[3], padded[4], padded[5])
    e_radial = lapse_factor * d_radial
    e_polar = lapse_factor * d_polar - shift_speed * b_azimuth
    e_azimuth = lapse_factor * d_azimuth + shift_speed * b_polar
    h_radial = lapse_factor * b_radial
    h_polar = lapse_factor * b_polar + shift_speed * d_azimuth
    h_azimuth = lapse_factor * b_azimuth - shift_speed * d_polar
    zeros_field = jnp.zeros_like(b_radial)
    radial_flux = jnp.stack([zeros_field, -e_azimuth, e_polar, zeros_field, h_azimuth, -h_polar])
    polar_flux = jnp.stack([e_azimuth, zeros_field, -e_radial, -h_azimuth, zeros_field, h_radial])
    azimuth_flux = jnp.stack([-e_polar, e_radial, zeros_field, h_polar, -h_radial, zeros_field])
    radial_faces = face_fluxes(radial_flux[:, :, 3:-3, 3:-3], padded[:, :, 3:-3, 3:-3], 0)
    polar_faces = face_fluxes(polar_flux[:, 3:-3, :, 3:-3], padded[:, 3:-3, :, 3:-3], 1)
    azimuth_faces = face_fluxes(azimuth_flux[:, 3:-3, 3:-3, :], padded[:, 3:-3, 3:-3, :], 2)
    radius_face = (0.5 * (radii[2:-3] + radii[3:-2])) ** 2
    radius_cell = radii[3:-3] ** 2
    sine_face = jnp.sin(0.5 * (angles[2:-3] + angles[3:-2]))
    sine_cell = jnp.sin(angles[3:-3])
    radial_div = (radius_face[None, 1:, None, None] * radial_faces[:, 1:] - radius_face[None, :-1, None, None] * radial_faces[:, :-1]) / (radius_cell[None, :, None, None] * spacing_r)
    polar_div = (sine_face[None, None, 1:, None] * polar_faces[:, :, 1:] - sine_face[None, None, :-1, None] * polar_faces[:, :, :-1]) / (sine_cell[None, None, :, None] * spacing_theta)
    azimuth_div = (azimuth_faces[:, :, :, 1:] - azimuth_faces[:, :, :, :-1]) / spacing_phi
    return -(radial_div + polar_div + azimuth_div)

def project(fields):
    magnetic_part = fields[:3]
    electric_part = fields[3:]
    b_square = jnp.maximum(lax.optimization_barrier(jnp.sum(magnetic_part * magnetic_part, axis=0)), 1.0)
    along = lax.optimization_barrier(jnp.sum(magnetic_part * electric_part, axis=0)) / b_square
    electric_part = electric_part - along[None] * magnetic_part
    d_square = lax.optimization_barrier(jnp.sum(electric_part * electric_part, axis=0))
    shrink = jnp.sqrt(b_square / jnp.maximum(d_square, b_square))
    return jnp.concatenate([magnetic_part, electric_part * shrink[None]], axis=0)

def extend(fields):
    grown = jnp.pad(fields, ((0, 0), (3, 3), (0, 0), (0, 0)))
    parity = jnp.array([1.0, -1.0, -1.0, 1.0, -1.0, -1.0], jnp.float32)[:, None, None, None]
    half_turn = grown.shape[3] // 2
    north_rows = jnp.roll(grown[:, :, 2::-1, :], half_turn, axis=3) * parity
    south_rows = jnp.roll(grown[:, :, :-4:-1, :], half_turn, axis=3) * parity
    grown = jnp.concatenate([north_rows, grown, south_rows], axis=2)
    return jnp.concatenate([grown[..., -3:], grown, grown[..., :3]], axis=3)

def reference(magnetic, electric):
    fields = jnp.concatenate([magnetic, electric], axis=0)
    spacing_theta = math.pi / NT
    spacing_r = spacing_theta
    spacing_phi = 2.0 * math.pi / NP
    step_dt = courant / (1.0 / spacing_r + 1.0 / spacing_theta + 1.0 / spacing_phi)
    radii = inner_radius + (jnp.arange(-3, NR + 3).astype(jnp.float32) + 0.5) * spacing_r
    angles = (jnp.arange(-3, NT + 3).astype(jnp.float32) + 0.5) * spacing_theta
    current = fields
    for weight in (0.0, 0.75, 1.0 / 3.0):
        rates = tendency(extend(current), radii, angles, spacing_r, spacing_theta, spacing_phi)
        current = project(weight * fields + (1.0 - weight) * (current + step_dt * rates))
    return (current[:3], current[3:])
```

```python
import functools
import math

import jax
import jax.numpy as jnp
from jax import lax
from jax.experimental import pallas as pl
from jax.experimental.pallas import tpu as pltpu
from jax.sharding import PartitionSpec as P

MESH = pl.DeviceIdType.MESH
hole_mass = 1.0
inner_radius = 1.8
wave_speed = 1.25
courant = 0.3
smooth_eps = 1e-06
G = 3

AXES = ((1, 2, 4, 5, 0, 3), (0, 2, 3, 5, 1, 4))
PAD = 1


def kept(make):
    made = {}

    def get(i):
        if i not in made:
            made[i] = make(i)
        return made[i]

    return get


class Line:
    def __init__(self, v):
        self.v = v
        self.d = kept(lambda i: v(i + 1) - v(i))
        self.e = kept(lambda i: self.d(i) * self.d(i))
        self.ee = kept(lambda i: self.e(i) + 3.0 * smooth_eps)
        self.f = kept(lambda i: 2.5 * self.e(i))
        self.p = kept(lambda i: self.d(i - 1) * self.d(i))
        self.b = kept(lambda i: 2.75 * self.p(i))
        self.step = kept(lambda i: self.d(i) - self.d(i - 1))
        self.t = kept(lambda i: self.step(i + 1) - self.step(i))
        self.tt = kept(lambda i: self.t(i) + self.t(i))
        self.low = kept(lambda i: self.weight((self.ee(i - 1) + self.f(i)) - self.b(i)))
        self.mid = kept(lambda i: 6.0 * self.weight((self.ee(i - 1) + self.e(i)) - 1.25 * self.p(i)))
        self.high = kept(lambda i: self.weight((self.ee(i) + self.f(i - 1)) - self.b(i)))

    def weight(self, smooth):
        q = pl.reciprocal(smooth, approx=True)
        return q * q

    def up(self, c):
        return self.blend(self.low(c - 1), self.mid(c), 3.0 * self.high(c + 1), self.tt(c - 1), self.t(c))

    def down(self, c):
        return self.blend(self.high(c + 2), self.mid(c + 1), 3.0 * self.low(c), self.tt(c + 1), self.t(c))

    def blend(self, w0, w1, w2, t0, t2):
        den = (w0 + w2) + w1
        return (w0 * t0 + w2 * t2) * pl.reciprocal(den, approx=True)


def faces(k, f, which):
    k = kept(k)
    if f is None:
        line = Line(k)
        for i in which:
            c = i + 2
            yield i, line.t(c) - (line.up(c) + line.down(c))
        return
    f = kept(f)
    plus, minus = Line(kept(lambda i: f(i) + k(i))), Line(kept(lambda i: f(i) - k(i)))
    f10, f4, f2 = (kept(lambda i, x=x: x * f(i)) for x in (10.0, 4.0, 2.0))
    for i in which:
        c = i + 2
        lin = ((f10(c) + f4(c + 1)) - f2(c - 1)) - minus.t(c)
        yield i, lin - (plus.up(c) - minus.down(c))


def kernel(sizes, mag, ele, mag_out, ele_out, u, te, tr, pe, pr, tt, dd, kr, fr, kt, ft, gr, gt, acc,
           ca, cs, car, csr, crp, crm, cth, lane_a, lane_s, send, recv, local):
    n_row, n_theta, n_phi, nr, nt, L = sizes
    row, th, ph = lax.axis_index("row"), lax.axis_index("theta"), lax.axis_index("phi")
    halves = nt // 8
    spacing = math.pi / (nt * n_theta)
    spacing_phi = 2.0 * math.pi / (L * n_phi)
    dt = courant / (1.0 / spacing + 1.0 / spacing + 1.0 / spacing_phi)
    scale = -dt / 12.0
    coef_phi = scale / spacing_phi
    planes = nr + 2 * G
    rows6, rows4 = 6 * nr, 4 * nr
    full, rest = L // nt, nr - L // nt
    seg = L // 8
    jump = seg + PAD
    first_row = 16
    blocks = pe.shape[3]
    te_rows = te.reshape(3, 2, 8 * rows6, L)
    pe_rows = pe.reshape(3, 2, 8 * blocks, L)
    pr_rows = pr.reshape(3, 2, 8 * blocks, L)

    def place(m):
        return m % seg + (m // seg) * jump

    first, last = th == 0, th == n_theta - 1
    opposite = (row, th, lax.rem(ph + n_phi // 2, n_phi))
    right = (row, th, lax.rem(ph + 1, n_phi))
    left = (row, th, lax.rem(ph + n_phi - 1, n_phi))
    above = tuple(jnp.where(last, o, q) for o, q in zip(opposite, (row, th + 1, ph)))
    below = tuple(jnp.where(first, o, q) for o, q in zip(opposite, (row, th - 1, ph)))
    outer, inner = (row + 1, th, ph), (row - 1, th, ph)
    has_outer, has_inner = row < n_row - 1, row > 0

    loads = [
        pltpu.make_async_copy(src, u.at[0, 3 * i : 3 * i + 3, G : G + nr], local.at[i])
        for i, src in enumerate((mag, ele))
    ]
    for c in loads:
        c.start()

    barrier = pltpu.get_barrier_semaphore()
    for target in (above, below, right, left):
        pl.semaphore_signal(barrier, inc=1, device_id=target, device_id_type=MESH)

    @pl.when(has_outer)
    def _():
        pl.semaphore_signal(barrier, inc=1, device_id=outer, device_id_type=MESH)

    @pl.when(has_inner)
    def _():
        pl.semaphore_signal(barrier, inc=1, device_id=inner, device_id_type=MESH)

    lane = lax.broadcasted_iota(jnp.int32, (8, L), 1)
    sub = lax.broadcasted_iota(jnp.int32, (8, L), 0)

    def radius_at(index):
        return inner_radius + (index.astype(jnp.float32) + 0.5) * spacing

    def lapse_shift(radius):
        ratio = 2.0 * hole_mass / radius
        return 1.0 / jnp.sqrt(1.0 + ratio), ratio / (1.0 + ratio)

    for r0 in (0, nr - 8):
        a, s = lapse_shift(radius_at(row * nr + r0 + sub))
        car[r0 : r0 + 8] = a
        csr[r0 : r0 + 8] = s

    def tables(q, carry):
        index = jnp.full((8, L), row * nr - G + q, jnp.int32)
        a, s = lapse_shift(radius_at(index))
        ca[q] = a
        cs[q] = s
        rc, hi, lo = radius_at(index), radius_at(index + 1), radius_at(index - 1)
        area = scale / (rc * rc * spacing)
        crp[q] = (0.5 * (rc + hi)) ** 2 * area
        crm[q] = (0.5 * (rc + lo)) ** 2 * area
        return carry

    lax.fori_loop(0, planes, tables, 0)
    for q in range(halves):
        index = (th * nt + 8 * q + sub).astype(jnp.float32)
        mid = jnp.sin((index + 0.5) * spacing)
        cth[0, 8 * q : 8 * q + 8] = scale * jnp.sin((index + 1.0) * spacing) / (mid * spacing)
        cth[1, 8 * q : 8 * q + 8] = scale * jnp.sin(index * spacing) / (mid * spacing)

    def owner(x, size):
        out = jnp.zeros((8, L), jnp.int32)
        for q in range(1, L // size):
            out = out + (x >= size * q).astype(jnp.int32)
        return out

    a, s = lapse_shift(radius_at(row * nr + owner(lane, nt)))
    lane_a[0], lane_a[1] = a, -a
    lane_s[0], lane_s[1] = s, s
    second = lane >= L // 2
    a, s = lapse_shift(radius_at(row * nr + full + owner(jnp.where(second, lane - L // 2, lane), nt)))
    lane_a[2], lane_s[2] = jnp.where(second, -a, a), s

    zeros = jnp.zeros((nt, L), jnp.float32)
    for stage in range(3):
        @pl.when(row == 0)
        def _():
            for c in range(6):
                for q in range(G):
                    u[stage, c, q] = zeros

        @pl.when(row == n_row - 1)
        def _():
            for c in range(6):
                for q in range(G):
                    u[stage, c, G + nr + q] = zeros

    def radial_flux(x, a, s):
        b2, b3, d2, d3 = x[1], x[2], x[4], x[5]
        return [-(a * d3 + s * b2), a * d2 - s * b3, a * b3 - s * d2, -(a * b2 + s * d3)]

    def polar_flux(x, a, s):
        b1, b2, b3, d1, d2, d3 = x
        return [a * d3 + s * b2, -(a * d1), s * d2 - a * b3, a * b1]

    def prepare(stage, r, tiles):
        a, s = ca[r + G], cs[r + G]
        for t in range(halves):
            rows = slice(8 * t, 8 * t + 8)
            x = [tiles[c][t] for c in range(6)]
            k = [wave_speed * y for y in x]
            for l, y in enumerate(radial_flux(x, a, s)):
                fr[l, r + G, rows] = y
            for l, c in enumerate(AXES[0]):
                kr[l, r + G, rows] = k[c]
            for l, y in enumerate(polar_flux(x, a, s)):
                ft[pl.ds((G + 8 * t) * rows4 + l * nr + r, 8, stride=rows4), :] = y
            for l, c in enumerate(AXES[1]):
                kt[pl.ds((G + 8 * t) * rows6 + l * nr + r, 8, stride=rows6), :] = k[c]
            for side, edge in enumerate((0, halves - 1)):
                if t == edge:
                    for c in range(6):
                        te_rows[stage, side, pl.ds(c * nr + r, 8, stride=rows6), :] = x[c]

    def turn(stage, out, parts):
        x = [u[stage, c, G + p : G + p + n].reshape(n * nt, L) for c, p, n in parts]
        x = (x[0] if len(x) == 1 else jnp.concatenate(x, axis=0)).T
        for q in range(L // 8):
            tt[out, pl.ds(first_row + place(8 * q), 8), :] = x[8 * q : 8 * q + 8]
        pe_rows[stage, 0, pl.ds(out, 8, stride=blocks), :] = x[0:8]
        pe_rows[stage, 1, pl.ds(out, 8, stride=blocks), :] = x[L - 8 : L]

    def turn_all(stage):
        for c in range(6):
            turn(stage, c, [(c, 0, full)])
        for c in range(3):
            turn(stage, 6 + c, [(c, full, rest), (3 + c, full, rest)])
        for c in range(2):
            turn(stage, 9 + c, [(3 + c, full, rest), (c, full, rest)])

    def remote(src, dst, stage, m_send, m_recv, target):
        return pltpu.make_async_remote_copy(
            src_ref=src, dst_ref=dst, send_sem=send.at[stage, m_send], recv_sem=recv.at[stage, m_recv],
            device_id=target, device_id_type=MESH,
        )

    def radial_out(stage):
        return remote(u.at[stage, :, nr : nr + G], u.at[stage, :, 0:G], stage, 0, 0, outer)

    def radial_in(stage):
        return remote(u.at[stage, :, G : 2 * G], u.at[stage, :, G + nr : nr + 2 * G], stage, 1, 1, inner)

    def theta_copies(stage):
        up = jnp.where(last, 1, 0)
        down = jnp.where(first, 0, 1)
        return (
            remote(te.at[stage, 1, 8 - G : 8], tr.at[stage, up], stage, 2, 2 + up, above),
            remote(te.at[stage, 0, 0:G], tr.at[stage, down], stage, 3, 2 + down, below),
        )

    def phi_copies(stage):
        return (
            remote(pe.at[stage, 1, 8 - G : 8], pr.at[stage, 0, 8 - G : 8], stage, 4, 4, right),
            remote(pe.at[stage, 0, 0:G], pr.at[stage, 1, 0:G], stage, 5, 5, left),
        )

    def send_all(stage):
        @pl.when(has_outer)
        def _():
            radial_out(stage).start()

        @pl.when(has_inner)
        def _():
            radial_in(stage).start()

        for c in theta_copies(stage):
            c.start()
        turn_all(stage)
        for c in phi_copies(stage):
            c.start()

    for c in loads:
        c.wait()

    def prepare_first(r, carry):
        prepare(0, r, [[u[0, c, r + G, 8 * t : 8 * t + 8] for t in range(halves)] for c in range(6)])
        return carry

    lax.fori_loop(0, nr, prepare_first, 0)
    pl.semaphore_wait(barrier, 4 + jnp.where(has_outer, 1, 0) + jnp.where(has_inner, 1, 0))
    send_all(0)

    def radial_faces(which):
        def part(t, carry):
            rows = pl.ds(pl.multiple_of(8 * t, 8), 8)
            for l in range(6):
                k = lambda i: kr[l, i, rows]
                f = (lambda i: fr[l, i, rows]) if l < 4 else None
                for span in which:
                    for i, x in faces(k, f, span):
                        gr[l, i, rows] = x
            return carry

        lax.fori_loop(0, halves, part, 0)

    def polar_faces(which):
        def part(q, carry):
            for j in range(3):
                v = 2 * q + j if j < 2 else 2 * (nr // 4) + q
                k = lambda i: kt[pl.ds(pl.multiple_of(i * rows6 + 8 * v, 8), 8), :]
                f = (lambda i: ft[pl.ds(pl.multiple_of(i * rows4 + 8 * v, 8), 8), :]) if j < 2 else None
                for span in which:
                    for i, x in faces(k, f, span):
                        gt[pl.ds(pl.multiple_of(i * rows6 + 8 * v, 8), 8), :] = x
            return carry

        lax.fori_loop(0, nr // 4, part, 0)

    def azimuth_faces():
        def part(q, carry):
            a, s = lane_a[q], lane_s[q]
            swapped = jnp.where(q == 0, 3, jnp.where(q == 1, 0, 9))

            def at(block, i):
                return tt[block, pl.ds(first_row + place(i - G), 8, stride=jump), :]

            own = [kept(lambda i, c=c: at(3 * q + c, i)) for c in range(3)]
            fluxes = (
                lambda i: s * own[2](i) - a * at(swapped + 1, i),
                lambda i: a * at(swapped, i),
                None,
            )
            for c in range(3):
                before = None
                for i, x in faces(lambda i: wave_speed * own[c](i), fluxes[c], range(seg + 1)):
                    if i:
                        dd[3 * q + c, pl.ds(i - 1, 8, stride=jump), :] = coef_phi * (x - before)
                    before = x
            return carry

        lax.fori_loop(0, 3, part, 0)

    def turn_back():
        for b in range(9):
            x = jnp.concatenate([dd[b, pl.ds(place(8 * q), 8), :] for q in range(L // 8)], axis=0).T
            if b < 6:
                acc[b, 0:full] = x.reshape(full, nt, L)
            else:
                x = x.reshape(2 * rest, nt, L)
                acc[b - 6, full:nr] = x[:rest]
                acc[b - 3, full:nr] = x[rest:]

    inside_r = (range(G, nr - G + 1),)
    edges_r = (range(0, G), range(nr - G + 1, nr + 1))
    inside_t = (range(G, nt - G + 1),)
    edges_t = (range(0, G), range(nt - G + 1, nt + 1))

    def stage_body(stage, carry):
        radial_faces(inside_r)
        polar_faces(inside_t)

        for c in phi_copies(stage):
            c.wait_recv()
        for b in range(11):
            tt[b, pl.ds(first_row + place(-G) - (8 - G), 8), :] = pr_rows[stage, 0, pl.ds(b, 8, stride=blocks), :]
            tt[b, pl.ds(first_row + place(L), 8), :] = pr_rows[stage, 1, pl.ds(b, 8, stride=blocks), :]
        azimuth_faces()
        turn_back()

        @pl.when(has_inner)
        def _():
            radial_out(stage).wait_recv()

        @pl.when(has_outer)
        def _():
            radial_in(stage).wait_recv()

        def ghost_planes(q, carry):
            p = jnp.where(q < G, q, q + nr)
            a, s = ca[p], cs[p]
            for t in range(halves):
                rows = slice(8 * t, 8 * t + 8)
                x = [u[stage, c, p, rows] for c in range(6)]
                for l, y in enumerate(radial_flux(x, a, s)):
                    fr[l, p, rows] = y
                for l, c in enumerate(AXES[0]):
                    kr[l, p, rows] = wave_speed * x[c]
            return carry

        lax.fori_loop(0, 2 * G, ghost_planes, 0)
        radial_faces(edges_r)

        for side in range(2):
            remote(te.at[stage, side, 0:G], tr.at[stage, side], stage, 2, 2 + side, above).wait_recv()
            pole = first if side == 0 else last
            sign = jnp.where(pole, -1.0, 1.0)
            for g in range(G):
                k = jnp.where(pole, G - 1 - g, g)
                target = g if side == 0 else G + nt + g
                for r0 in (0, nr - 8):
                    a, s = car[r0 : r0 + 8], csr[r0 : r0 + 8]
                    x = [tr[stage, side, k, c * nr + r0 : c * nr + r0 + 8] for c in range(6)]
                    x = [y * sign if c % 3 else y for c, y in enumerate(x)]
                    for l, y in enumerate(polar_flux(x, a, s)):
                        ft[pl.ds(target * rows4 + l * nr + r0, 8), :] = y
                    for l, c in enumerate(AXES[1]):
                        kt[pl.ds(target * rows6 + l * nr + r0, 8), :] = wave_speed * x[c]
        polar_faces(edges_t)

        w = jnp.where(stage == 0, 0.0, jnp.where(stage == 1, 0.75, 1.0 / 3.0)).astype(jnp.float32)

        def update(r):
            rp, rm = crp[r + G], crm[r + G]
            new = [[None] * halves for _ in range(6)]
            for t in range(halves):
                rows = slice(8 * t, 8 * t + 8)
                for c in range(6):
                    lr, lt = AXES[0].index(c), AXES[1].index(c)
                    low = gt[pl.ds(8 * t * rows6 + lt * nr + r, 8, stride=rows6), :]
                    high = gt[pl.ds((8 * t + 1) * rows6 + lt * nr + r, 8, stride=rows6), :]
                    rate = acc[c, r, rows] + (cth[0, rows] * high - cth[1, rows] * low)
                    rate = rate + (rp * gr[lr, r + 1, rows] - rm * gr[lr, r, rows])
                    new[c][t] = w * u[0, c, r + G, rows] + (1.0 - w) * (u[stage, c, r + G, rows] + rate)
                b, d = [new[c][t] for c in range(3)], [new[c][t] for c in range(3, 6)]
                b2 = jnp.maximum(b[0] * b[0] + b[1] * b[1] + b[2] * b[2], 1.0)
                along = (b[0] * d[0] + b[1] * d[1] + b[2] * d[2]) * pl.reciprocal(b2, approx=True)
                d = [y - along * x for x, y in zip(b, d)]
                d2 = d[0] * d[0] + d[1] * d[1] + d[2] * d[2]
                shrink = b2 * lax.rsqrt(b2 * jnp.maximum(d2, b2))
                for c in range(3):
                    new[3 + c][t] = d[c] * shrink
                for c in range(6):
                    u[stage + 1, c, r + G, rows] = new[c][t]
            return new

        pair = 2 if nr % 2 == 0 else 1

        def final(i, carry):
            new = [update(pair * i + j) for j in range(pair)]

            @pl.when(stage < 2)
            def _():
                for j in range(pair):
                    prepare(stage + 1, pair * i + j, new[j])

            return carry

        lax.fori_loop(0, nr // pair, final, 0)

        @pl.when(stage < 2)
        def _():
            send_all(stage + 1)

        return carry

    lax.fori_loop(0, 3, stage_body, 0)
    stores = [
        pltpu.make_async_copy(u.at[3, 3 * i : 3 * i + 3, G : G + nr], dst, local.at[i])
        for i, dst in enumerate((mag_out, ele_out))
    ]
    for c in stores:
        c.start()

    def drain(stage, carry):
        @pl.when(has_outer)
        def _():
            radial_out(stage).wait_send()

        @pl.when(has_inner)
        def _():
            radial_in(stage).wait_send()

        for c in theta_copies(stage) + phi_copies(stage):
            c.wait_send()
        return carry

    lax.fori_loop(0, 3, drain, 0)
    for c in stores:
        c.wait()


def solution(mesh):
    n_row, n_theta, n_phi = (mesh.shape[k] for k in ("row", "theta", "phi"))

    def body(magnetic, electric):
        _, nr, nt, lanes = magnetic.shape
        planes = nr + 2 * G
        pad8 = lambda n: -(-n // 8) * 8
        f32 = jnp.float32
        vm = lambda *shape: pltpu.VMEM(shape, f32)
        assert nt % 8 == 0 and nr % 4 == 0 and 2 * nr * nt == 3 * lanes
        long = lanes + 8 * PAD
        sizes = (n_row, n_theta, n_phi, nr, nt, lanes)
        anywhere = pl.BlockSpec(memory_space=pl.ANY)
        return pl.pallas_call(
            functools.partial(kernel, sizes),
            out_shape=[jax.ShapeDtypeStruct(magnetic.shape, f32)] * 2,
            in_specs=[anywhere] * 2,
            out_specs=[anywhere] * 2,
            scratch_shapes=[
                vm(4, 6, planes, nt, lanes),
                vm(3, 2, 8, 6 * nr, lanes),
                vm(3, 2, G, 6 * nr, lanes),
                vm(3, 2, 8, 16, lanes),
                vm(3, 2, 8, 16, lanes),
                vm(11, 16 + pad8(long) + 8, lanes),
                vm(9, pad8(long), lanes),
                vm(6, planes, nt, lanes),
                vm(4, planes, nt, lanes),
                vm((nt + 2 * G) * 6 * nr, lanes),
                vm((nt + 2 * G) * 4 * nr, lanes),
                vm(6, nr + 1, nt, lanes),
                vm((nt + 1) * 6 * nr, lanes),
                vm(6, nr, nt, lanes),
                vm(planes, 8, lanes),
                vm(planes, 8, lanes),
                vm(pad8(nr), lanes),
                vm(pad8(nr), lanes),
                vm(planes, 8, lanes),
                vm(planes, 8, lanes),
                vm(2, nt, lanes),
                vm(3, 8, lanes),
                vm(3, 8, lanes),
                pltpu.SemaphoreType.DMA((3, 6)),
                pltpu.SemaphoreType.DMA((3, 6)),
                pltpu.SemaphoreType.DMA((2,)),
            ],
            compiler_params=pltpu.CompilerParams(
                collective_id=0, has_side_effects=True
            ),
        )(magnetic, electric)

    spec = P(None, "row", "theta", "phi")
    return jax.shard_map(body, mesh=mesh, in_specs=(spec, spec), out_specs=(spec, spec), check_vma=False)
```

```python
import functools
import math

import jax
import jax.numpy as jnp
from jax import lax
from jax.experimental import pallas as pl
from jax.experimental.pallas import tpu as pltpu
from jax.sharding import PartitionSpec as P

MESH = pl.DeviceIdType.MESH
hole_mass = 1.0
inner_radius = 1.8
wave_speed = 1.25
courant = 0.3
smooth_eps = 1e-06
G = 3

AXES = ((1, 2, 4, 5, 0, 3), (0, 2, 3, 5, 1, 4))
PAD = 1


def kept(make):
    made = {}

    def get(i):
        if i not in made:
            made[i] = make(i)
        return made[i]

    return get


class Line:
    def __init__(self, v):
        self.v = v
        self.d = kept(lambda i: v(i + 1) - v(i))
        self.e = kept(lambda i: self.d(i) * self.d(i))
        self.ee = kept(lambda i: self.e(i) + 3.0 * smooth_eps)
        self.f = kept(lambda i: 2.5 * self.e(i))
        self.p = kept(lambda i: self.d(i - 1) * self.d(i))
        self.b = kept(lambda i: 2.75 * self.p(i))
        self.step = kept(lambda i: self.d(i) - self.d(i - 1))
        self.t = kept(lambda i: self.step(i + 1) - self.step(i))
        self.tt = kept(lambda i: self.t(i) + self.t(i))
        self.low = kept(lambda i: self.weight((self.ee(i - 1) + self.f(i)) - self.b(i)))
        self.mid = kept(lambda i: 6.0 * self.weight((self.ee(i - 1) + self.e(i)) - 1.25 * self.p(i)))
        self.high = kept(lambda i: self.weight((self.ee(i) + self.f(i - 1)) - self.b(i)))

    def weight(self, smooth):
        q = pl.reciprocal(smooth, approx=True)
        return q * q

    def up(self, c):
        return self.blend(self.low(c - 1), self.mid(c), 3.0 * self.high(c + 1), self.tt(c - 1), self.t(c))

    def down(self, c):
        return self.blend(self.high(c + 2), self.mid(c + 1), 3.0 * self.low(c), self.tt(c + 1), self.t(c))

    def blend(self, w0, w1, w2, t0, t2):
        den = (w0 + w2) + w1
        return (w0 * t0 + w2 * t2) * pl.reciprocal(den, approx=True)


def faces(k, f, which):
    k = kept(k)
    if f is None:
        line = Line(k)
        for i in which:
            c = i + 2
            yield i, line.t(c) - (line.up(c) + line.down(c))
        return
    f = kept(f)
    plus, minus = Line(kept(lambda i: f(i) + k(i))), Line(kept(lambda i: f(i) - k(i)))
    f10, f4, f2 = (kept(lambda i, x=x: x * f(i)) for x in (10.0, 4.0, 2.0))
    for i in which:
        c = i + 2
        lin = ((f10(c) + f4(c + 1)) - f2(c - 1)) - minus.t(c)
        yield i, lin - (plus.up(c) - minus.down(c))


def kernel(sizes, mag, ele, mag_out, ele_out, u, te, tr, pe, pr, tt, dd, kr, fr, kt, ft, gr, gt, ga, acc,
           ca, cs, car, csr, crp, crm, cth, lane_a, lane_s, send, recv, local):
    n_row, n_theta, n_phi, nr, nt, L = sizes
    row, th, ph = lax.axis_index("row"), lax.axis_index("theta"), lax.axis_index("phi")
    halves = nt // 8
    spacing = math.pi / (nt * n_theta)
    spacing_phi = 2.0 * math.pi / (L * n_phi)
    dt = courant / (1.0 / spacing + 1.0 / spacing + 1.0 / spacing_phi)
    scale = -dt / 12.0
    coef_phi = scale / spacing_phi
    planes = nr + 2 * G
    rows6, rows4 = 6 * nr, 4 * nr
    pitch6, pitch4 = rows6 + PAD, rows4 + PAD
    full, rest = L // nt, nr - L // nt
    seg = L // 8
    jump = seg + PAD
    first_row = 16
    blocks = pe.shape[3]
    te_rows = te.reshape(3, 2, 8 * rows6, L)
    pe_rows = pe.reshape(3, 2, 8 * blocks, L)
    pr_rows = pr.reshape(3, 2, 8 * blocks, L)

    def place(m):
        return m % seg + (m // seg) * jump

    first, last = th == 0, th == n_theta - 1
    opposite = (row, th, lax.rem(ph + n_phi // 2, n_phi))
    right = (row, th, lax.rem(ph + 1, n_phi))
    left = (row, th, lax.rem(ph + n_phi - 1, n_phi))
    above = tuple(jnp.where(last, o, q) for o, q in zip(opposite, (row, th + 1, ph)))
    below = tuple(jnp.where(first, o, q) for o, q in zip(opposite, (row, th - 1, ph)))
    outer, inner = (row + 1, th, ph), (row - 1, th, ph)
    has_outer, has_inner = row < n_row - 1, row > 0

    loads = [
        pltpu.make_async_copy(src, u.at[0, 3 * i : 3 * i + 3, G : G + nr], local.at[i])
        for i, src in enumerate((mag, ele))
    ]
    for c in loads:
        c.start()

    barrier = pltpu.get_barrier_semaphore()
    for target in (above, below, right, left):
        pl.semaphore_signal(barrier, inc=1, device_id=target, device_id_type=MESH)

    @pl.when(has_outer)
    def _():
        pl.semaphore_signal(barrier, inc=1, device_id=outer, device_id_type=MESH)

    @pl.when(has_inner)
    def _():
        pl.semaphore_signal(barrier, inc=1, device_id=inner, device_id_type=MESH)

    lane = lax.broadcasted_iota(jnp.int32, (8, L), 1)
    sub = lax.broadcasted_iota(jnp.int32, (8, L), 0)

    def radius_at(index):
        return inner_radius + (index.astype(jnp.float32) + 0.5) * spacing

    def lapse_shift(radius):
        ratio = 2.0 * hole_mass / radius
        return 1.0 / jnp.sqrt(1.0 + ratio), ratio / (1.0 + ratio)

    for r0 in (0, nr - 8):
        a, s = lapse_shift(radius_at(row * nr + r0 + sub))
        car[r0 : r0 + 8] = a
        csr[r0 : r0 + 8] = s

    def tables(q, carry):
        index = jnp.full((8, L), row * nr - G + q, jnp.int32)
        a, s = lapse_shift(radius_at(index))
        ca[q] = a
        cs[q] = s
        rc, hi, lo = radius_at(index), radius_at(index + 1), radius_at(index - 1)
        area = scale / (rc * rc * spacing)
        crp[q] = (0.5 * (rc + hi)) ** 2 * area
        crm[q] = (0.5 * (rc + lo)) ** 2 * area
        return carry

    lax.fori_loop(0, planes, tables, 0)
    for q in range(halves):
        index = (th * nt + 8 * q + sub).astype(jnp.float32)
        mid = jnp.sin((index + 0.5) * spacing)
        cth[0, 8 * q : 8 * q + 8] = scale * jnp.sin((index + 1.0) * spacing) / (mid * spacing)
        cth[1, 8 * q : 8 * q + 8] = scale * jnp.sin(index * spacing) / (mid * spacing)

    def owner(x, size):
        out = jnp.zeros((8, L), jnp.int32)
        for q in range(1, L // size):
            out = out + (x >= size * q).astype(jnp.int32)
        return out

    a, s = lapse_shift(radius_at(row * nr + owner(lane, nt)))
    lane_a[0], lane_a[1] = a, -a
    lane_s[0], lane_s[1] = s, s
    second = lane >= L // 2
    a, s = lapse_shift(radius_at(row * nr + full + owner(jnp.where(second, lane - L // 2, lane), nt)))
    lane_a[2], lane_s[2] = jnp.where(second, -a, a), s

    zeros = jnp.zeros((nt, L), jnp.float32)
    for stage in range(3):
        @pl.when(row == 0)
        def _():
            for c in range(6):
                for q in range(G):
                    u[stage, c, q] = zeros

        @pl.when(row == n_row - 1)
        def _():
            for c in range(6):
                for q in range(G):
                    u[stage, c, G + nr + q] = zeros

    def radial_flux(x, a, s):
        b2, b3, d2, d3 = x[1], x[2], x[4], x[5]
        return [-(a * d3 + s * b2), a * d2 - s * b3, a * b3 - s * d2, -(a * b2 + s * d3)]

    def polar_flux(x, a, s):
        b1, b2, b3, d1, d2, d3 = x
        return [a * d3 + s * b2, -(a * d1), s * d2 - a * b3, a * b1]

    def prepare(stage, r, tiles):
        a, s = ca[r + G], cs[r + G]
        for t in range(halves):
            rows = slice(8 * t, 8 * t + 8)
            x = [tiles[c][t] for c in range(6)]
            k = [wave_speed * y for y in x]
            for l, y in enumerate(radial_flux(x, a, s)):
                fr[l, r + G, rows] = y
            for l, c in enumerate(AXES[0]):
                kr[l, r + G, rows] = k[c]
            for l, y in enumerate(polar_flux(x, a, s)):
                ft[pl.ds((G + 8 * t) * pitch4 + l * nr + r, 8, stride=pitch4), :] = y
            for l, c in enumerate(AXES[1]):
                kt[pl.ds((G + 8 * t) * pitch6 + l * nr + r, 8, stride=pitch6), :] = k[c]
            for side, edge in enumerate((0, halves - 1)):
                if t == edge:
                    for c in range(6):
                        te_rows[stage, side, pl.ds(c * nr + r, 8, stride=rows6), :] = x[c]

    def turn(stage, out, parts):
        x = [u[stage, c, G + p : G + p + n].reshape(n * nt, L) for c, p, n in parts]
        x = (x[0] if len(x) == 1 else jnp.concatenate(x, axis=0)).T
        for q in range(L // 8):
            tt[out, pl.ds(first_row + place(8 * q), 8), :] = x[8 * q : 8 * q + 8]
        pe_rows[stage, 0, pl.ds(out, 8, stride=blocks), :] = x[0:8]
        pe_rows[stage, 1, pl.ds(out, 8, stride=blocks), :] = x[L - 8 : L]

    def turn_all(stage):
        for c in range(6):
            turn(stage, c, [(c, 0, full)])
        for c in range(3):
            turn(stage, 6 + c, [(c, full, rest), (3 + c, full, rest)])
        for c in range(2):
            turn(stage, 9 + c, [(3 + c, full, rest), (c, full, rest)])

    def remote(src, dst, stage, m_send, m_recv, target):
        return pltpu.make_async_remote_copy(
            src_ref=src, dst_ref=dst, send_sem=send.at[stage, m_send], recv_sem=recv.at[stage, m_recv],
            device_id=target, device_id_type=MESH,
        )

    def radial_out(stage):
        return remote(u.at[stage, :, nr : nr + G], u.at[stage, :, 0:G], stage, 0, 0, outer)

    def radial_in(stage):
        return remote(u.at[stage, :, G : 2 * G], u.at[stage, :, G + nr : nr + 2 * G], stage, 1, 1, inner)

    def theta_copies(stage):
        up = jnp.where(last, 1, 0)
        down = jnp.where(first, 0, 1)
        return (
            remote(te.at[stage, 1, 8 - G : 8], tr.at[stage, up], stage, 2, 2 + up, above),
            remote(te.at[stage, 0, 0:G], tr.at[stage, down], stage, 3, 2 + down, below),
        )

    def phi_copies(stage):
        return (
            remote(pe.at[stage, 1, 8 - G : 8], pr.at[stage, 0, 8 - G : 8], stage, 4, 4, right),
            remote(pe.at[stage, 0, 0:G], pr.at[stage, 1, 0:G], stage, 5, 5, left),
        )

    def send_all(stage):
        @pl.when(has_outer)
        def _():
            radial_out(stage).start()

        @pl.when(has_inner)
        def _():
            radial_in(stage).start()

        turn_all(stage)
        for c in phi_copies(stage) + theta_copies(stage):
            c.start()

    for c in loads:
        c.wait()

    def prepare_first(r, carry):
        prepare(0, r, [[u[0, c, r + G, 8 * t : 8 * t + 8] for t in range(halves)] for c in range(6)])
        return carry

    lax.fori_loop(0, nr, prepare_first, 0)
    pl.semaphore_wait(barrier, 4 + jnp.where(has_outer, 1, 0) + jnp.where(has_inner, 1, 0))
    send_all(0)

    def radial_faces(which):
        def part(t, carry):
            rows = pl.ds(pl.multiple_of(8 * t, 8), 8)
            for l in range(6):
                k = lambda i: kr[l, i, rows]
                f = (lambda i: fr[l, i, rows]) if l < 4 else None
                for span in which:
                    for i, x in faces(k, f, span):
                        gr[l, i, rows] = x
            return carry

        lax.fori_loop(0, halves, part, 0)

    def polar_faces(which):
        def part(q, carry):
            for j in range(3):
                v = 2 * q + j if j < 2 else 2 * (nr // 4) + q
                k = lambda i: kt[pl.ds(i * pitch6 + 8 * v, 8), :]
                f = (lambda i: ft[pl.ds(i * pitch4 + 8 * v, 8), :]) if j < 2 else None
                for span in which:
                    for i, x in faces(k, f, span):
                        gt[pl.ds(i * pitch6 + 8 * v, 8), :] = x
            return carry

        lax.fori_loop(0, nr // 4, part, 0)

    def azimuth_faces(which):
        def part(q, carry):
            a, s = lane_a[q], lane_s[q]
            swapped = jnp.where(q == 0, 3, jnp.where(q == 1, 0, 9))

            def at(block, i):
                return tt[block, pl.ds(first_row + place(i - G), 8, stride=jump), :]

            own = [kept(lambda i, c=c: at(3 * q + c, i)) for c in range(3)]
            fluxes = (
                lambda i: s * own[2](i) - a * at(swapped + 1, i),
                lambda i: a * at(swapped, i),
                None,
            )
            for c in range(3):
                k = lambda i: wave_speed * own[c](i)
                for span in which:
                    before = None
                    for i, x in faces(k, fluxes[c], span):
                        if i == G or i == seg - G:
                            ga[3 * q + c, int(i != G)] = x
                        if before is None and i == seg - G + 1:
                            before = ga[3 * q + c, 1]
                        if before is not None:
                            dd[3 * q + c, pl.ds(i - 1, 8, stride=jump), :] = coef_phi * (x - before)
                        before = x
                    if span[-1] == G - 1:
                        dd[3 * q + c, pl.ds(G - 1, 8, stride=jump), :] = coef_phi * (ga[3 * q + c, 0] - before)
            return carry

        lax.fori_loop(0, 3, part, 0)

    def turn_back():
        for b in range(9):
            x = jnp.concatenate([dd[b, pl.ds(place(8 * q), 8), :] for q in range(L // 8)], axis=0).T
            if b < 6:
                acc[b, 0:full] = x.reshape(full, nt, L)
            else:
                x = x.reshape(2 * rest, nt, L)
                acc[b - 6, full:nr] = x[:rest]
                acc[b - 3, full:nr] = x[rest:]

    inside_r = (range(G, nr - G + 1),)
    edges_r = (range(0, G), range(nr - G + 1, nr + 1))
    inside_t = (range(G, nt - G + 1),)
    inside_a = (range(G, seg - G + 1),)
    edges_a = (range(0, G), range(seg - G + 1, seg + 1))
    edges_t = (range(0, G), range(nt - G + 1, nt + 1))

    def stage_body(stage, carry):
        radial_faces(inside_r)
        polar_faces(inside_t)
        azimuth_faces(inside_a)

        for c in phi_copies(stage):
            c.wait_recv()
        for b in range(11):
            tt[b, pl.ds(first_row + place(-G) - (8 - G), 8), :] = pr_rows[stage, 0, pl.ds(b, 8, stride=blocks), :]
            tt[b, pl.ds(first_row + place(L), 8), :] = pr_rows[stage, 1, pl.ds(b, 8, stride=blocks), :]
        azimuth_faces(edges_a)
        turn_back()

        @pl.when(has_inner)
        def _():
            radial_out(stage).wait_recv()

        @pl.when(has_outer)
        def _():
            radial_in(stage).wait_recv()

        def ghost_planes(q, carry):
            p = jnp.where(q < G, q, q + nr)
            a, s = ca[p], cs[p]
            for t in range(halves):
                rows = slice(8 * t, 8 * t + 8)
                x = [u[stage, c, p, rows] for c in range(6)]
                for l, y in enumerate(radial_flux(x, a, s)):
                    fr[l, p, rows] = y
                for l, c in enumerate(AXES[0]):
                    kr[l, p, rows] = wave_speed * x[c]
            return carry

        lax.fori_loop(0, 2 * G, ghost_planes, 0)
        radial_faces(edges_r)

        for side in range(2):
            remote(te.at[stage, side, 0:G], tr.at[stage, side], stage, 2, 2 + side, above).wait_recv()
            pole = first if side == 0 else last
            sign = jnp.where(pole, -1.0, 1.0)
            for g in range(G):
                k = jnp.where(pole, G - 1 - g, g)
                target = g if side == 0 else G + nt + g
                for r0 in (0, nr - 8):
                    a, s = car[r0 : r0 + 8], csr[r0 : r0 + 8]
                    x = [tr[stage, side, k, c * nr + r0 : c * nr + r0 + 8] for c in range(6)]
                    x = [y * sign if c % 3 else y for c, y in enumerate(x)]
                    for l, y in enumerate(polar_flux(x, a, s)):
                        ft[pl.ds(target * pitch4 + l * nr + r0, 8), :] = y
                    for l, c in enumerate(AXES[1]):
                        kt[pl.ds(target * pitch6 + l * nr + r0, 8), :] = wave_speed * x[c]
        polar_faces(edges_t)

        w = jnp.where(stage == 0, 0.0, jnp.where(stage == 1, 0.75, 1.0 / 3.0)).astype(jnp.float32)

        def update(r):
            rp, rm = crp[r + G], crm[r + G]
            new = [[None] * halves for _ in range(6)]
            for t in range(halves):
                rows = slice(8 * t, 8 * t + 8)
                for c in range(6):
                    lr, lt = AXES[0].index(c), AXES[1].index(c)
                    low = gt[pl.ds(8 * t * pitch6 + lt * nr + r, 8, stride=pitch6), :]
                    high = gt[pl.ds((8 * t + 1) * pitch6 + lt * nr + r, 8, stride=pitch6), :]
                    rate = acc[c, r, rows] + (cth[0, rows] * high - cth[1, rows] * low)
                    rate = rate + (rp * gr[lr, r + 1, rows] - rm * gr[lr, r, rows])
                    new[c][t] = w * u[0, c, r + G, rows] + (1.0 - w) * (u[stage, c, r + G, rows] + rate)
                b, d = [new[c][t] for c in range(3)], [new[c][t] for c in range(3, 6)]
                b2 = jnp.maximum(b[0] * b[0] + b[1] * b[1] + b[2] * b[2], 1.0)
                along = (b[0] * d[0] + b[1] * d[1] + b[2] * d[2]) * pl.reciprocal(b2, approx=True)
                d = [y - along * x for x, y in zip(b, d)]
                d2 = d[0] * d[0] + d[1] * d[1] + d[2] * d[2]
                shrink = b2 * lax.rsqrt(b2 * jnp.maximum(d2, b2))
                for c in range(3):
                    new[3 + c][t] = d[c] * shrink
            return new

        pair = 2 if nr % 2 == 0 else 1

        def final(i, carry):
            new = [update(pair * i + j) for j in range(pair)]

            @pl.when(stage < 2)
            def _():
                for j in range(pair):
                    for c in range(6):
                        for t in range(halves):
                            u[stage + 1, c, pair * i + j + G, 8 * t : 8 * t + 8] = new[j][c][t]
                    prepare(stage + 1, pair * i + j, new[j])

            @pl.when(stage == 2)
            def _():
                for j in range(pair):
                    for c in range(3):
                        for t in range(halves):
                            mag_out[c, pair * i + j, 8 * t : 8 * t + 8] = new[j][c][t]
                            ele_out[c, pair * i + j, 8 * t : 8 * t + 8] = new[j][3 + c][t]

            return carry

        lax.fori_loop(0, nr // pair, final, 0)

        @pl.when(stage < 2)
        def _():
            send_all(stage + 1)

        return carry

    lax.fori_loop(0, 3, stage_body, 0)
    def drain(stage, carry):
        @pl.when(has_outer)
        def _():
            radial_out(stage).wait_send()

        @pl.when(has_inner)
        def _():
            radial_in(stage).wait_send()

        for c in theta_copies(stage) + phi_copies(stage):
            c.wait_send()
        return carry

    lax.fori_loop(0, 3, drain, 0)


def solution(mesh):
    n_row, n_theta, n_phi = (mesh.shape[k] for k in ("row", "theta", "phi"))

    def put_out(m, e, mo, eo, sem):
        copies = [pltpu.make_async_copy(x, y, sem.at[i]) for i, (x, y) in enumerate(((m, mo), (e, eo)))]
        for c in copies:
            c.start()
        for c in copies:
            c.wait()

    def body(magnetic, electric):
        _, nr, nt, lanes = magnetic.shape
        planes = nr + 2 * G
        pad8 = lambda n: -(-n // 8) * 8
        f32 = jnp.float32
        vm = lambda *shape: pltpu.VMEM(shape, f32)
        assert nt % 8 == 0 and nr % 4 == 0 and 2 * nr * nt == 3 * lanes
        long = lanes + 8 * PAD
        sizes = (n_row, n_theta, n_phi, nr, nt, lanes)
        anywhere = pl.BlockSpec(memory_space=pl.ANY)
        out = pl.pallas_call(
            functools.partial(kernel, sizes),
            out_shape=[pltpu.VMEM(magnetic.shape, f32)] * 2,
            in_specs=[anywhere] * 2,
            out_specs=[pl.BlockSpec(memory_space=pltpu.VMEM)] * 2,
            scratch_shapes=[
                vm(3, 6, planes, nt, lanes),
                vm(3, 2, 8, 6 * nr, lanes),
                vm(3, 2, G, 6 * nr, lanes),
                vm(3, 2, 8, 16, lanes),
                vm(3, 2, 8, 16, lanes),
                vm(11, 16 + pad8(long) + 8, lanes),
                vm(9, pad8(long), lanes),
                vm(6, planes, nt, lanes),
                vm(4, planes, nt, lanes),
                vm(pad8((nt + 2 * G) * (6 * nr + PAD)), lanes),
                vm(pad8((nt + 2 * G) * (4 * nr + PAD)), lanes),
                vm(6, nr + 1, nt, lanes),
                vm(pad8((nt + 1) * (6 * nr + PAD)), lanes),
                vm(9, 2, 8, lanes),
                vm(6, nr, nt, lanes),
                vm(planes, 8, lanes),
                vm(planes, 8, lanes),
                vm(pad8(nr), lanes),
                vm(pad8(nr), lanes),
                vm(planes, 8, lanes),
                vm(planes, 8, lanes),
                vm(2, nt, lanes),
                vm(3, 8, lanes),
                vm(3, 8, lanes),
                pltpu.SemaphoreType.DMA((3, 6)),
                pltpu.SemaphoreType.DMA((3, 6)),
                pltpu.SemaphoreType.DMA((2,)),
            ],
            compiler_params=pltpu.CompilerParams(
                collective_id=0, has_side_effects=True
            ),
        )(magnetic, electric)
        return pl.pallas_call(
            put_out,
            out_shape=[jax.ShapeDtypeStruct(magnetic.shape, f32)] * 2,
            in_specs=[pl.BlockSpec(memory_space=pltpu.VMEM)] * 2,
            out_specs=[anywhere] * 2,
            scratch_shapes=[pltpu.SemaphoreType.DMA((2,))],
            compiler_params=pltpu.CompilerParams(vmem_limit_bytes=4 * 2**20),
        )(*out)

    spec = P(None, "row", "theta", "phi")
    return jax.shard_map(body, mesh=mesh, in_specs=(spec, spec), out_specs=(spec, spec), check_vma=False)
```

```python
import functools
import math

import jax
import jax.numpy as jnp
from jax import lax
from jax.experimental import pallas as pl
from jax.experimental.pallas import tpu as pltpu
from jax.sharding import PartitionSpec as P

MESH = pl.DeviceIdType.MESH
hole_mass = 1.0
inner_radius = 1.8
wave_speed = 1.25
courant = 0.3
smooth_eps = 1e-06
G = 3

AXES = ((1, 2, 4, 5, 0, 3), (0, 2, 3, 5, 1, 4))
PAD = 1


def kept(make):
    made = {}

    def get(i):
        if i not in made:
            made[i] = make(i)
        return made[i]

    return get


class Line:
    def __init__(self, v):
        self.v = v
        self.d = kept(lambda i: v(i + 1) - v(i))
        self.e = kept(lambda i: self.d(i) * self.d(i) + 4.0 * smooth_eps)
        self.e4 = kept(lambda i: 4.0 * self.e(i))
        self.step = kept(lambda i: self.d(i) - self.d(i - 1))
        self.s2 = kept(lambda i: self.step(i) * self.step(i))
        self.t = kept(lambda i: self.step(i + 1) - self.step(i))
        self.t2 = kept(lambda i: 0.5 * self.t(i))
        self.sum = kept(lambda i: self.e(i - 1) + self.e(i))
        self.rest = kept(lambda i: (11.0 / 3.0) * self.s2(i) - self.sum(i))
        self.mid = kept(lambda i: self.sum(i) + (5.0 / 3.0) * self.s2(i))
        self.low = kept(lambda i: self.rest(i) + self.e4(i))
        self.high = kept(lambda i: self.rest(i) + self.e4(i - 1))
        self.w_low, self.w_mid, self.w_high = (
            kept(lambda i, x=x: self.weight(x(i))) for x in (self.low, self.mid, self.high)
        )
        self.mid6 = kept(lambda i: 6.0 * self.w_mid(i))

    def weight(self, smooth):
        q = pl.reciprocal(smooth, approx=True)
        return q * q

    def up(self, c):
        return ratio(self.low(c - 1), self.mid(c), self.high(c + 1), self.t(c - 1), self.t2(c))

    def down(self, c):
        return ratio(self.high(c + 2), self.mid(c + 1), self.low(c), self.t(c + 1), self.t2(c))

    def both(self, c):
        return blend(
            self.w_low(c - 1), self.mid6(c), 3.0 * self.w_high(c + 1), self.t(c - 1), self.t2(c)
        ) + blend(
            self.w_high(c + 2), self.mid6(c + 1), 3.0 * self.w_low(c), self.t(c + 1), self.t2(c)
        )


def blend(w0, w1, w2, t0, t2):
    den = (w0 + w2) + w1
    return (w0 * t0 + w2 * t2) * pl.reciprocal(den, approx=True)


def ratio(s0, s1, s2, t0, t2):
    y0, y2 = s1 * pl.reciprocal(s0, approx=True), s1 * pl.reciprocal(s2, approx=True)
    return blend(y0 * y0, 6.0, 3.0 * (y2 * y2), t0, t2)


def faces(p, m, f, which):
    line = Line(kept(p))
    if m is None:
        for i in which:
            c = i + 2
            yield i, line.t2(c) - line.both(c)
        return
    other = Line(kept(m))
    f = kept(f)
    f5, f2 = kept(lambda i: 5.0 * f(i)), kept(lambda i: f(i) + f(i))
    for i in which:
        c = i + 2
        lin = (f5(c) + (f2(c + 1) - f(c - 1))) - other.t2(c)
        yield i, lin - (line.up(c) - other.down(c))


def kernel(sizes, mag, ele, mag_out, ele_out, u, ta, tb, ra, rb, pa, pb, qa, qb, tt, dd, vr, vt, gr, gt, ga, acc,
           ca, cs, car, csr, crp, crm, cth, lane_a, lane_s, send, recv, local):
    n_row, n_theta, n_phi, nr, nt, L = sizes
    row, th, ph = lax.axis_index("row"), lax.axis_index("theta"), lax.axis_index("phi")
    halves = nt // 8
    spacing = math.pi / (nt * n_theta)
    spacing_phi = 2.0 * math.pi / (L * n_phi)
    dt = courant / (1.0 / spacing + 1.0 / spacing + 1.0 / spacing_phi)
    scale = -dt / 6.0
    coef_phi = scale / spacing_phi
    planes = nr + 2 * G
    rows6, rows14 = 6 * nr, 14 * nr
    pitch6, pitch14 = rows6 + PAD, rows14 + PAD
    full, rest = L // nt, nr - L // nt
    seg = L // 8
    jump = seg + PAD
    first_row = 16
    sent = ((pa, qa, 0, 6, 24), (pb, qb, 6, 3, 16))
    early = 2 * rest
    groups = ((0, early), (early, rest))
    ta_rows = ta.reshape(3, 2, 8 * 6 * early, L)
    tb_rows = tb.reshape(3, 2, 8 * 6 * rest, L)

    def spot(l, q, late, lines=14):
        return lines * early + l * rest + q - early if late else l * early + q

    def plane_of(q):
        return q + full if isinstance(q, int) and q < rest else (
            q - rest if isinstance(q, int) else jnp.where(q < rest, q + full, q - rest))

    def place(m):
        return m % seg + (m // seg) * jump

    first, last = th == 0, th == n_theta - 1
    opposite = (row, th, lax.rem(ph + n_phi // 2, n_phi))
    right = (row, th, lax.rem(ph + 1, n_phi))
    left = (row, th, lax.rem(ph + n_phi - 1, n_phi))
    above = tuple(jnp.where(last, o, q) for o, q in zip(opposite, (row, th + 1, ph)))
    below = tuple(jnp.where(first, o, q) for o, q in zip(opposite, (row, th - 1, ph)))
    outer, inner = (row + 1, th, ph), (row - 1, th, ph)
    has_outer, has_inner = row < n_row - 1, row > 0

    loads = [
        pltpu.make_async_copy(src, u.at[0, 3 * i : 3 * i + 3, G : G + nr], local.at[i])
        for i, src in enumerate((mag, ele))
    ]
    for c in loads:
        c.start()

    barrier = pltpu.get_barrier_semaphore()
    for target in (above, below, right, left):
        pl.semaphore_signal(barrier, inc=1, device_id=target, device_id_type=MESH)

    @pl.when(has_outer)
    def _():
        pl.semaphore_signal(barrier, inc=1, device_id=outer, device_id_type=MESH)

    @pl.when(has_inner)
    def _():
        pl.semaphore_signal(barrier, inc=1, device_id=inner, device_id_type=MESH)

    lane = lax.broadcasted_iota(jnp.int32, (8, L), 1)
    sub = lax.broadcasted_iota(jnp.int32, (8, L), 0)

    def radius_at(index):
        return inner_radius + (index.astype(jnp.float32) + 0.5) * spacing

    def lapse_shift(radius):
        ratio = 2.0 * hole_mass / radius
        return 1.0 / jnp.sqrt(1.0 + ratio), ratio / (1.0 + ratio)

    for i, (q0, _) in enumerate(groups):
        index = q0 + sub
        a, s = lapse_shift(radius_at(row * nr + jnp.where(index < rest, index + full, index - rest)))
        car[8 * i : 8 * i + 8] = a
        csr[8 * i : 8 * i + 8] = s

    def tables(q, carry):
        index = jnp.full((8, L), row * nr - G + q, jnp.int32)
        a, s = lapse_shift(radius_at(index))
        ca[q] = a
        cs[q] = s
        rc, hi, lo = radius_at(index), radius_at(index + 1), radius_at(index - 1)
        area = scale / (rc * rc * spacing)
        crp[q] = (0.5 * (rc + hi)) ** 2 * area
        crm[q] = (0.5 * (rc + lo)) ** 2 * area
        return carry

    lax.fori_loop(0, planes, tables, 0)
    for q in range(halves):
        index = (th * nt + 8 * q + sub).astype(jnp.float32)
        mid = jnp.sin((index + 0.5) * spacing)
        cth[0, 8 * q : 8 * q + 8] = scale * jnp.sin((index + 1.0) * spacing) / (mid * spacing)
        cth[1, 8 * q : 8 * q + 8] = scale * jnp.sin(index * spacing) / (mid * spacing)

    def owner(x, size):
        out = jnp.zeros((8, L), jnp.int32)
        for q in range(1, L // size):
            out = out + (x >= size * q).astype(jnp.int32)
        return out

    index = owner(lane, nt)
    a, s = lapse_shift(radius_at(row * nr + jnp.where(index < rest, index + full, index - rest)))
    lane_a[0], lane_a[1] = a, -a
    lane_s[0], lane_s[1] = s, s
    second = lane >= L // 2
    a, s = lapse_shift(radius_at(row * nr + rest + owner(jnp.where(second, lane - L // 2, lane), nt)))
    lane_a[2], lane_s[2] = jnp.where(second, -a, a), s

    zeros = jnp.zeros((nt, L), jnp.float32)
    for stage in range(3):
        @pl.when(row == 0)
        def _():
            for c in range(6):
                for q in range(G):
                    u[stage, c, q] = zeros

        @pl.when(row == n_row - 1)
        def _():
            for c in range(6):
                for q in range(G):
                    u[stage, c, G + nr + q] = zeros

    def radial_flux(x, a, s):
        b2, b3, d2, d3 = x[1], x[2], x[4], x[5]
        return [-(a * d3 + s * b2), a * d2 - s * b3, a * b3 - s * d2, -(a * b2 + s * d3)]

    def polar_flux(x, a, s):
        b1, b2, b3, d1, d2, d3 = x
        return [a * d3 + s * b2, -(a * d1), s * d2 - a * b3, a * b1]

    def lines(dim, x, f):
        k = [wave_speed * y for y in x]
        two = [k[c] for c in AXES[dim][:4]]
        return (
            [y + z for y, z in zip(f, two)] + [y - z for y, z in zip(f, two)] + f + [k[c] for c in AXES[dim][4:]]
        )

    def prepare(stage, q, r, tiles, late):
        a, s = ca[r + G], cs[r + G]
        for t in range(halves):
            rows = slice(8 * t, 8 * t + 8)
            x = [tiles[c][t] for c in range(6)]
            for l, y in enumerate(lines(0, x, radial_flux(x, a, s))):
                vr[l, r + G, rows] = y
            for l, y in enumerate(lines(1, x, polar_flux(x, a, s))):
                vt[pl.ds((G + 8 * t) * pitch14 + spot(l, q, late), 8, stride=pitch14), :] = y
            for side, end in enumerate((0, halves - 1)):
                if t == end:
                    for c in range(6):
                        if late:
                            tb_rows[stage, side, pl.ds(c * rest + q - early, 8, stride=6 * rest), :] = x[c]
                        else:
                            ta_rows[stage, side, pl.ds(c * early + q, 8, stride=6 * early), :] = x[c]

    def turn(stage, out, parts):
        x = jnp.concatenate([u[stage, c, G + p : G + p + n].reshape(n * nt, L) for c, p, n in parts], axis=0).T
        for q in range(L // 8):
            tt[out, pl.ds(first_row + place(8 * q), 8), :] = x[8 * q : 8 * q + 8]
        for src, _, b, n, _ in sent:
            if b <= out < b + n:
                src[stage, 0, pl.ds(out - b, 8, stride=n), :] = x[0:8]
                src[stage, 1, pl.ds(out - b, 8, stride=n), :] = x[L - 8 : L]

    def turn_early(stage):
        for c in range(6):
            turn(stage, c, [(c, full, rest), (c, 0, full - rest)])

    def turn_late(stage):
        p = full - rest
        for c in range(3):
            turn(stage, 6 + c, [(c, p, rest), (3 + c, p, rest)])
        for c in range(2):
            turn(stage, 9 + c, [(3 + c, p, rest), (c, p, rest)])

    def remote(src, dst, stage, m_send, m_recv, target):
        return pltpu.make_async_remote_copy(
            src_ref=src, dst_ref=dst, send_sem=send.at[stage, m_send], recv_sem=recv.at[stage, m_recv],
            device_id=target, device_id_type=MESH,
        )

    def radial_out(stage):
        return remote(u.at[stage, :, nr : nr + G], u.at[stage, :, 0:G], stage, 0, 0, outer)

    def radial_in(stage):
        return remote(u.at[stage, :, G : 2 * G], u.at[stage, :, G + nr : nr + 2 * G], stage, 1, 1, inner)

    def theta_copies(stage, late):
        up = jnp.where(last, 1, 0)
        down = jnp.where(first, 0, 1)
        src, dst = (tb, rb) if late else (ta, ra)
        base = 6 if late else 2
        return (
            remote(src.at[stage, 1, 8 - G : 8], dst.at[stage, up], stage, base, base + up, above),
            remote(src.at[stage, 0, 0:G], dst.at[stage, down], stage, base + 1, base + down, below),
        )

    def phi_copies(stage, late):
        src, dst, _, n, edge = sent[late]
        head, tail = pl.ds(0, edge), pl.ds(8 * n - edge, edge)
        base = 8 if late else 4
        return (
            remote(src.at[stage, 1, tail], dst.at[stage, 0, tail], stage, base, base, right),
            remote(src.at[stage, 0, head], dst.at[stage, 1, head], stage, base + 1, base + 1, left),
        )

    def send_early(stage):
        @pl.when(has_outer)
        def _():
            radial_out(stage).start()

        @pl.when(has_inner)
        def _():
            radial_in(stage).start()

        turn_early(stage)
        for c in phi_copies(stage, False) + theta_copies(stage, False):
            c.start()

    def send_late(stage):
        turn_late(stage)
        for c in phi_copies(stage, True) + theta_copies(stage, True):
            c.start()

    for c in loads:
        c.wait()

    def prepare_first(late):
        def part(q, carry):
            r = plane_of(q)
            tiles = [[u[0, c, r + G, 8 * t : 8 * t + 8] for t in range(halves)] for c in range(6)]
            prepare(0, q, r, tiles, late)
            return carry

        return part

    lax.fori_loop(0, early, prepare_first(False), 0)
    lax.fori_loop(early, nr, prepare_first(True), 0)
    pl.semaphore_wait(barrier, 4 + jnp.where(has_outer, 1, 0) + jnp.where(has_inner, 1, 0))
    send_early(0)
    send_late(0)

    def radial_faces(which):
        def part(t, carry):
            rows = pl.ds(pl.multiple_of(8 * t, 8), 8)
            for l in range(6):
                at = lambda j: lambda i: vr[j, i, rows]
                parts = (at(l), at(l + 4), at(l + 8)) if l < 4 else (at(l + 8), None, None)
                for span in which:
                    for i, x in faces(*parts, span):
                        gr[l, i, rows] = x
            return carry

        lax.fori_loop(0, halves, part, 0)

    def polar_faces(lo, hi, which, also):
        def part(q, carry):
            late = lo == 2
            n = rest if late else early
            for j in range(3):
                v = (0 if late else (1 + (j < 2)) * q) + (j if j < 2 else 0)
                base = 14 * early if late else 0
                at = lambda m: lambda i: vt[pl.ds(i * pitch14 + base + 4 * n * m + 8 * v, 8), :]
                parts = (at(0), at(1), at(2)) if j < 2 else (at(3), None, None)
                out = (6 * early if late else 0) + (4 * n if j == 2 else 0) + 8 * v
                for span in which:
                    for i, x in faces(*parts, span):
                        gt[pl.ds(i * pitch6 + out, 8), :] = x
                if also is not None:
                    also(q, j)
            return carry

        lax.fori_loop(lo, hi, part, 0)

    def azimuth_faces(lo, hi, which):
        def part(q, carry):
            a, s = lane_a[q], lane_s[q]
            swapped = jnp.where(q == 0, 3, jnp.where(q == 1, 0, 9))

            def at(block, i):
                return tt[block, pl.ds(first_row + place(i - G), 8, stride=jump), :]

            own = [kept(lambda i, c=c: at(3 * q + c, i)) for c in range(3)]
            fluxes = (
                lambda i: s * own[2](i) - a * at(swapped + 1, i),
                lambda i: a * at(swapped, i),
                None,
            )
            for c in range(3):
                k = kept(lambda i: wave_speed * own[c](i))
                f = kept(fluxes[c]) if fluxes[c] else None
                parts = (lambda i: f(i) + k(i), lambda i: f(i) - k(i), f) if f else (k, None, None)
                for span in which:
                    before = None
                    for i, x in faces(*parts, span):
                        if span[0] == G and (i == G or i == seg - G):
                            ga[3 * q + c, int(i != G)] = x
                        if span[0] == i == seg - G + 1:
                            before = ga[3 * q + c, 1]
                        if before is not None:
                            dd[3 * q + c, pl.ds(i - 1, 8, stride=jump), :] = coef_phi * (x - before)
                        before = x
                    if span == range(0, G):
                        dd[3 * q + c, pl.ds(G - 1, 8, stride=jump), :] = coef_phi * (ga[3 * q + c, 0] - before)
            return carry

        lax.fori_loop(lo, hi, part, 0)

    def turn_back(q, j):
        b = 3 * q + j
        x = jnp.concatenate([dd[b, pl.ds(place(8 * i), 8), :] for i in range(L // 8)], axis=0).T
        acc[b] = x.reshape(full, nt, L)

    inside_r = (range(G, nr - G + 1),)
    edges_r = (range(0, G), range(nr - G + 1, nr + 1))
    inside_t = (range(G, nt - G + 1),)
    inside_a = (range(G, seg - G + 1),)
    edges_a = (range(0, G), range(seg - G + 1, seg + 1))
    edges_t = (range(0, G), range(nt - G + 1, nt + 1))
    whole_t, whole_a = (range(nt + 1),), (range(seg + 1),)

    def azimuth_ghosts(stage, late):
        for c in phi_copies(stage, late):
            c.wait_recv()
        before, after = first_row + place(-G) - (8 - G), first_row + place(L)
        _, dst, b0, n, _ = sent[late]
        for b in range(b0, b0 + n):
            x, y = (dst[stage, i, pl.ds(b - b0, 8, stride=n), :] for i in range(2))
            tt[b, pl.ds(before, 8), :] = x
            tt[b, pl.ds(after, 8), :] = y
            if 6 <= b < 8:
                tt[b + 3, pl.ds(before, 8), :] = pltpu.roll(x, L // 2, 1)
                tt[b + 3, pl.ds(after, 8), :] = pltpu.roll(y, L // 2, 1)

    def polar_ghosts(stage, late):
        src, dst, base = ((ta, ra, 2), (tb, rb, 6))[late]
        q0, n = groups[late]
        a, s = car[8 * late : 8 * late + n], csr[8 * late : 8 * late + n]
        for side in range(2):
            remote(src.at[stage, side, 0:G], dst.at[stage, side], stage, base, base + side, above).wait_recv()
            pole = first if side == 0 else last
            sign = jnp.where(pole, -1.0, 1.0)
            for g in range(G):
                k = jnp.where(pole, G - 1 - g, g)
                target = g if side == 0 else G + nt + g
                x = [dst[stage, side, k, c * n : c * n + n] for c in range(6)]
                x = [y * sign if c % 3 else y for c, y in enumerate(x)]
                for l, y in enumerate(lines(1, x, polar_flux(x, a, s))):
                    vt[pl.ds(target * pitch14 + spot(l, q0, late), n), :] = y

    def stage_body(stage, carry, ending=False):
        radial_faces(inside_r)
        polar_faces(0, 2, inside_t, None)
        azimuth_faces(0, 2, inside_a)

        azimuth_ghosts(stage, 0)
        azimuth_faces(0, 2, edges_a)
        @pl.when(has_inner)
        def _():
            radial_out(stage).wait_recv()

        @pl.when(has_outer)
        def _():
            radial_in(stage).wait_recv()

        def ghost_planes(q, carry):
            p = jnp.where(q < G, q, q + nr)
            a, s = ca[p], cs[p]
            for t in range(halves):
                rows = slice(8 * t, 8 * t + 8)
                x = [u[stage, c, p, rows] for c in range(6)]
                for l, y in enumerate(lines(0, x, radial_flux(x, a, s))):
                    vr[l, p, rows] = y
            return carry

        lax.fori_loop(0, 2 * G, ghost_planes, 0)
        radial_faces(edges_r)

        polar_ghosts(stage, 0)
        polar_faces(0, 2, edges_t, turn_back)

        w = jnp.where(stage == 0, 0.0, jnp.where(stage == 1, 0.75, 1.0 / 3.0)).astype(jnp.float32)

        def update(q, late):
            r = plane_of(q)
            rp, rm = crp[r + G], crm[r + G]
            new = [[None] * halves for _ in range(6)]
            for t in range(halves):
                rows = slice(8 * t, 8 * t + 8)
                for c in range(6):
                    lr, lt = AXES[0].index(c), AXES[1].index(c)
                    at = spot(lt, q, late, 6)
                    low = gt[pl.ds(8 * t * pitch6 + at, 8, stride=pitch6), :]
                    high = gt[pl.ds((8 * t + 1) * pitch6 + at, 8, stride=pitch6), :]
                    block, level = (6 + c % 3, q - early + rest * (c // 3)) if late else (c, q)
                    rate = acc[block, level, rows] + (cth[0, rows] * high - cth[1, rows] * low)
                    rate = rate + (rp * gr[lr, r + 1, rows] - rm * gr[lr, r, rows])
                    new[c][t] = w * u[0, c, r + G, rows] + (1.0 - w) * (u[stage, c, r + G, rows] + rate)
                b, d = [new[c][t] for c in range(3)], [new[c][t] for c in range(3, 6)]
                b2 = jnp.maximum(b[0] * b[0] + b[1] * b[1] + b[2] * b[2], 1.0)
                along = (b[0] * d[0] + b[1] * d[1] + b[2] * d[2]) * pl.reciprocal(b2, approx=True)
                d = [y - along * x for x, y in zip(b, d)]
                d2 = d[0] * d[0] + d[1] * d[1] + d[2] * d[2]
                shrink = b2 * lax.rsqrt(b2 * jnp.maximum(d2, b2))
                for c in range(3):
                    new[3 + c][t] = d[c] * shrink
            return new

        def keep(q, new, late):
            r = plane_of(q)
            for t in range(halves):
                rows = slice(8 * t, 8 * t + 8)
                for c in range(6):
                    if ending:
                        (mag_out, ele_out)[c // 3][c % 3, r, rows] = new[c][t]
                    else:
                        u[stage + 1, c, r + G, rows] = new[c][t]
            if not ending:
                prepare(stage + 1, q, r, new, late)

        def final(late, pair):
            def part(i, carry):
                new = [update(pair * i + j, late) for j in range(pair)]
                for j in range(pair):
                    keep(pair * i + j, new[j], late)
                return carry

            return part

        lax.fori_loop(0, early // 2, final(False, 2), 0)
        if not ending:
            send_early(stage + 1)
        azimuth_ghosts(stage, 1)
        azimuth_faces(2, 3, whole_a)
        polar_ghosts(stage, 1)
        polar_faces(2, 3, whole_t, turn_back)
        lax.fori_loop(early // 2, nr // 2, final(True, 2), 0)
        if not ending:
            send_late(stage + 1)
        return carry

    lax.fori_loop(0, 2, stage_body, 0)
    stage_body(2, 0, True)

    def drain(stage, carry):
        @pl.when(has_outer)
        def _():
            radial_out(stage).wait_send()

        @pl.when(has_inner)
        def _():
            radial_in(stage).wait_send()

        for c in theta_copies(stage, False) + theta_copies(stage, True) + phi_copies(stage, False) + phi_copies(stage, True):
            c.wait_send()
        return carry

    lax.fori_loop(0, 3, drain, 0)


def solution(mesh):
    n_row, n_theta, n_phi = (mesh.shape[k] for k in ("row", "theta", "phi"))

    def put_out(m, e, mo, eo, sem):
        copies = [pltpu.make_async_copy(x, y, sem.at[i]) for i, (x, y) in enumerate(((m, mo), (e, eo)))]
        for c in copies:
            c.start()
        for c in copies:
            c.wait()

    def body(magnetic, electric):
        _, nr, nt, lanes = magnetic.shape
        planes, rest = nr + 2 * G, nr - lanes // nt
        pad8 = lambda n: -(-n // 8) * 8
        f32 = jnp.float32
        vm = lambda *shape: pltpu.VMEM(shape, f32)
        assert nt % 8 == 0 and nr % 4 == 0 and 2 * nr * nt == 3 * lanes
        long = lanes + 8 * PAD
        sizes = (n_row, n_theta, n_phi, nr, nt, lanes)
        anywhere = pl.BlockSpec(memory_space=pl.ANY)
        out = pl.pallas_call(
            functools.partial(kernel, sizes),
            out_shape=[pltpu.VMEM(magnetic.shape, f32)] * 2,
            in_specs=[anywhere] * 2,
            out_specs=[pl.BlockSpec(memory_space=pltpu.VMEM)] * 2,
            scratch_shapes=[
                vm(3, 6, planes, nt, lanes),
                vm(3, 2, 8, 6 * 2 * rest, lanes),
                vm(3, 2, 8, 6 * rest, lanes),
                vm(3, 2, G, 6 * 2 * rest, lanes),
                vm(3, 2, G, 6 * rest, lanes),
                vm(3, 2, 8 * 6, lanes),
                vm(3, 2, 8 * 3, lanes),
                vm(3, 2, 8 * 6, lanes),
                vm(3, 2, 8 * 3, lanes),
                vm(11, 16 + pad8(long) + 8, lanes),
                vm(9, pad8(long), lanes),
                vm(14, planes, nt, lanes),
                vm(pad8((nt + 2 * G) * (14 * nr + PAD)), lanes),
                vm(6, nr + 1, nt, lanes),
                vm(pad8((nt + 1) * (6 * nr + PAD)), lanes),
                vm(9, 2, 8, lanes),
                vm(9, lanes // nt, nt, lanes),
                vm(planes, 8, lanes),
                vm(planes, 8, lanes),
                vm(16, lanes),
                vm(16, lanes),
                vm(planes, 8, lanes),
                vm(planes, 8, lanes),
                vm(2, nt, lanes),
                vm(3, 8, lanes),
                vm(3, 8, lanes),
                pltpu.SemaphoreType.DMA((3, 10)),
                pltpu.SemaphoreType.DMA((3, 10)),
                pltpu.SemaphoreType.DMA((2,)),
            ],
            compiler_params=pltpu.CompilerParams(
                collective_id=0, has_side_effects=True
            ),
        )(magnetic, electric)
        return pl.pallas_call(
            put_out,
            out_shape=[jax.ShapeDtypeStruct(magnetic.shape, f32)] * 2,
            in_specs=[pl.BlockSpec(memory_space=pltpu.VMEM)] * 2,
            out_specs=[anywhere] * 2,
            scratch_shapes=[pltpu.SemaphoreType.DMA((2,))],
            compiler_params=pltpu.CompilerParams(vmem_limit_bytes=4 * 2**20),
        )(*out)

    spec = P(None, "row", "theta", "phi")
    return jax.shard_map(body, mesh=mesh, in_specs=(spec, spec), out_specs=(spec, spec), check_vma=False)
```

```python
import functools
import math

import jax
import jax.numpy as jnp
from jax import lax
from jax.experimental import pallas as pl
from jax.experimental.pallas import tpu as pltpu
from jax.sharding import PartitionSpec as P

MESH = pl.DeviceIdType.MESH
hole_mass = 1.0
inner_radius = 1.8
wave_speed = 1.25
courant = 0.3
smooth_eps = 1e-06
G = 3

AXES = ((1, 2, 4, 5, 0, 3), (0, 2, 3, 5, 1, 4))
PAD = 1


def kept(make):
    made = {}

    def get(i):
        if i not in made:
            made[i] = make(i)
        return made[i]

    return get


class Line:
    def __init__(self, v):
        self.v = v
        self.d = kept(lambda i: v(i + 1) - v(i))
        self.e = kept(lambda i: self.d(i) * self.d(i) + 4.0 * smooth_eps)
        self.e4 = kept(lambda i: 4.0 * self.e(i))
        self.step = kept(lambda i: self.d(i) - self.d(i - 1))
        self.s2 = kept(lambda i: self.step(i) * self.step(i))
        self.t = kept(lambda i: self.step(i + 1) - self.step(i))
        self.t2 = kept(lambda i: 0.5 * self.t(i))
        self.sum = kept(lambda i: self.e(i - 1) + self.e(i))
        self.rest = kept(lambda i: (11.0 / 3.0) * self.s2(i) - self.sum(i))
        self.mid = kept(lambda i: self.sum(i) + (5.0 / 3.0) * self.s2(i))
        self.low = kept(lambda i: self.rest(i) + self.e4(i))
        self.high = kept(lambda i: self.rest(i) + self.e4(i - 1))
        self.w_low, self.w_mid, self.w_high = (
            kept(lambda i, x=x: self.weight(x(i))) for x in (self.low, self.mid, self.high)
        )
        self.mid6 = kept(lambda i: 6.0 * self.w_mid(i))

    def weight(self, smooth):
        q = pl.reciprocal(smooth, approx=True)
        return q * q

    def up(self, c):
        return ratio(self.low(c - 1), self.mid(c), self.high(c + 1), self.t(c - 1), self.t2(c))

    def down(self, c):
        return ratio(self.high(c + 2), self.mid(c + 1), self.low(c), self.t(c + 1), self.t2(c))

    def both(self, c):
        return blend(
            self.w_low(c - 1), self.mid6(c), 3.0 * self.w_high(c + 1), self.t(c - 1), self.t2(c)
        ) + blend(
            self.w_high(c + 2), self.mid6(c + 1), 3.0 * self.w_low(c), self.t(c + 1), self.t2(c)
        )


def blend(w0, w1, w2, t0, t2):
    den = (w0 + w2) + w1
    return (w0 * t0 + w2 * t2) * pl.reciprocal(den, approx=True)


def ratio(s0, s1, s2, t0, t2):
    y0, y2 = s1 * pl.reciprocal(s0, approx=True), s1 * pl.reciprocal(s2, approx=True)
    return blend(y0 * y0, 6.0, 3.0 * (y2 * y2), t0, t2)


def faces(p, m, f, which):
    line = Line(kept(p))
    if m is None:
        for i in which:
            c = i + 2
            yield i, line.t2(c) - line.both(c)
        return
    other = Line(kept(m))
    f = kept(f)
    f5, f2 = kept(lambda i: 5.0 * f(i)), kept(lambda i: f(i) + f(i))
    for i in which:
        c = i + 2
        lin = (f5(c) + (f2(c + 1) - f(c - 1))) - other.t2(c)
        yield i, lin - (line.up(c) - other.down(c))


def kernel(sizes, mag, ele, mag_out, ele_out, u, ta, tb, ra, rb, pa, pb, qa, qb, tt, dd, vr, vt, gr, gt, ga, acc,
           ca, cs, car, csr, crp, crm, cth, lane_a, lane_s, send, recv, local):
    n_row, n_theta, n_phi, nr, nt, L = sizes
    row, th, ph = lax.axis_index("row"), lax.axis_index("theta"), lax.axis_index("phi")
    halves = nt // 8
    spacing = math.pi / (nt * n_theta)
    spacing_phi = 2.0 * math.pi / (L * n_phi)
    dt = courant / (1.0 / spacing + 1.0 / spacing + 1.0 / spacing_phi)
    scale = -dt / 6.0
    coef_phi = scale / spacing_phi
    planes = nr + 2 * G
    rows6, rows14 = 6 * nr, 14 * nr
    pitch6, pitch14 = rows6 + PAD, rows14 + PAD
    full, rest = L // nt, nr - L // nt
    seg = L // 8
    jump = seg + PAD
    first_row = 16
    sent = ((pa, qa, 0, 6, 24), (pb, qb, 6, 3, 16))
    early = 2 * rest
    groups = ((0, early), (early, rest))
    ta_rows = ta.reshape(3, 2, 8 * 6 * early, L)
    tb_rows = tb.reshape(3, 2, 8 * 6 * rest, L)

    def spot(l, q, late, lines=14):
        return lines * early + l * rest + q - early if late else l * early + q

    def plane_of(q):
        return q + full if isinstance(q, int) and q < rest else (
            q - rest if isinstance(q, int) else jnp.where(q < rest, q + full, q - rest))

    def place(m):
        return m % seg + (m // seg) * jump

    first, last = th == 0, th == n_theta - 1
    opposite = (row, th, lax.rem(ph + n_phi // 2, n_phi))
    right = (row, th, lax.rem(ph + 1, n_phi))
    left = (row, th, lax.rem(ph + n_phi - 1, n_phi))
    above = tuple(jnp.where(last, o, q) for o, q in zip(opposite, (row, th + 1, ph)))
    below = tuple(jnp.where(first, o, q) for o, q in zip(opposite, (row, th - 1, ph)))
    outer, inner = (row + 1, th, ph), (row - 1, th, ph)
    has_outer, has_inner = row < n_row - 1, row > 0

    loads = [
        pltpu.make_async_copy(src, u.at[0, 3 * i : 3 * i + 3, G : G + nr], local.at[i])
        for i, src in enumerate((mag, ele))
    ]
    for c in loads:
        c.start()

    barrier = pltpu.get_barrier_semaphore()
    for target in (above, below, right, left):
        pl.semaphore_signal(barrier, inc=1, device_id=target, device_id_type=MESH)

    @pl.when(has_outer)
    def _():
        pl.semaphore_signal(barrier, inc=1, device_id=outer, device_id_type=MESH)

    @pl.when(has_inner)
    def _():
        pl.semaphore_signal(barrier, inc=1, device_id=inner, device_id_type=MESH)

    lane = lax.broadcasted_iota(jnp.int32, (8, L), 1)
    sub = lax.broadcasted_iota(jnp.int32, (8, L), 0)

    def radius_at(index):
        return inner_radius + (index.astype(jnp.float32) + 0.5) * spacing

    def lapse_shift(radius):
        ratio = 2.0 * hole_mass / radius
        return 1.0 / jnp.sqrt(1.0 + ratio), ratio / (1.0 + ratio)

    for i, (q0, _) in enumerate(groups):
        index = q0 + sub
        a, s = lapse_shift(radius_at(row * nr + jnp.where(index < rest, index + full, index - rest)))
        car[8 * i : 8 * i + 8] = a
        csr[8 * i : 8 * i + 8] = s

    def tables(q, carry):
        index = jnp.full((8, L), row * nr - G + q, jnp.int32)
        a, s = lapse_shift(radius_at(index))
        ca[q] = a
        cs[q] = s
        rc, hi, lo = radius_at(index), radius_at(index + 1), radius_at(index - 1)
        area = scale / (rc * rc * spacing)
        crp[q] = (0.5 * (rc + hi)) ** 2 * area
        crm[q] = (0.5 * (rc + lo)) ** 2 * area
        return carry

    lax.fori_loop(0, planes, tables, 0)
    for q in range(halves):
        index = (th * nt + 8 * q + sub).astype(jnp.float32)
        mid = jnp.sin((index + 0.5) * spacing)
        cth[0, 8 * q : 8 * q + 8] = scale * jnp.sin((index + 1.0) * spacing) / (mid * spacing)
        cth[1, 8 * q : 8 * q + 8] = scale * jnp.sin(index * spacing) / (mid * spacing)

    def owner(x, size):
        out = jnp.zeros((8, L), jnp.int32)
        for q in range(1, L // size):
            out = out + (x >= size * q).astype(jnp.int32)
        return out

    index = owner(lane, nt)
    a, s = lapse_shift(radius_at(row * nr + jnp.where(index < rest, index + full, index - rest)))
    lane_a[0], lane_a[1] = a, -a
    lane_s[0], lane_s[1] = s, s
    second = lane >= L // 2
    a, s = lapse_shift(radius_at(row * nr + rest + owner(jnp.where(second, lane - L // 2, lane), nt)))
    lane_a[2], lane_s[2] = jnp.where(second, -a, a), s

    zeros = jnp.zeros((nt, L), jnp.float32)
    for stage in range(3):
        @pl.when(row == 0)
        def _():
            for c in range(6):
                for q in range(G):
                    u[stage, c, q] = zeros

        @pl.when(row == n_row - 1)
        def _():
            for c in range(6):
                for q in range(G):
                    u[stage, c, G + nr + q] = zeros

    def radial_flux(x, a, s):
        b2, b3, d2, d3 = x[1], x[2], x[4], x[5]
        return [-(a * d3 + s * b2), a * d2 - s * b3, a * b3 - s * d2, -(a * b2 + s * d3)]

    def polar_flux(x, a, s):
        b1, b2, b3, d1, d2, d3 = x
        return [a * d3 + s * b2, -(a * d1), s * d2 - a * b3, a * b1]

    def lines(dim, x, f):
        k = [wave_speed * y for y in x]
        two = [k[c] for c in AXES[dim][:4]]
        return (
            [y + z for y, z in zip(f, two)] + [y - z for y, z in zip(f, two)] + f + [k[c] for c in AXES[dim][4:]]
        )

    def prepare(stage, q, r, tiles, late):
        a, s = ca[r + G], cs[r + G]
        for t in range(halves):
            rows = slice(8 * t, 8 * t + 8)
            x = [tiles[c][t] for c in range(6)]
            for l, y in enumerate(lines(0, x, radial_flux(x, a, s))):
                vr[l, r + G, rows] = y
            for l, y in enumerate(lines(1, x, polar_flux(x, a, s))):
                vt[pl.ds((G + 8 * t) * pitch14 + spot(l, q, late), 8, stride=pitch14), :] = y
            for side, end in enumerate((0, halves - 1)):
                if t == end:
                    for c in range(6):
                        if late:
                            tb_rows[stage, side, pl.ds(c * rest + q - early, 8, stride=6 * rest), :] = x[c]
                        else:
                            ta_rows[stage, side, pl.ds(c * early + q, 8, stride=6 * early), :] = x[c]

    def turn(stage, out, parts):
        x = jnp.concatenate([u[stage, c, G + p : G + p + n].reshape(n * nt, L) for c, p, n in parts], axis=0).T
        for q in range(L // 8):
            tt[out, pl.ds(first_row + place(8 * q), 8), :] = x[8 * q : 8 * q + 8]
        for src, _, b, n, _ in sent:
            if b <= out < b + n:
                src[stage, 0, pl.ds(out - b, 8, stride=n), :] = x[0:8]
                src[stage, 1, pl.ds(out - b, 8, stride=n), :] = x[L - 8 : L]

    def turn_early(stage):
        for c in range(6):
            turn(stage, c, [(c, full, rest), (c, 0, full - rest)])

    def turn_late(stage):
        p = full - rest
        for c in range(3):
            turn(stage, 6 + c, [(c, p, rest), (3 + c, p, rest)])
        for c in range(2):
            turn(stage, 9 + c, [(3 + c, p, rest), (c, p, rest)])

    def remote(src, dst, stage, m_send, m_recv, target):
        return pltpu.make_async_remote_copy(
            src_ref=src, dst_ref=dst, send_sem=send.at[stage, m_send], recv_sem=recv.at[stage, m_recv],
            device_id=target, device_id_type=MESH,
        )

    def radial_out(stage):
        return remote(u.at[stage, :, nr : nr + G], u.at[stage, :, 0:G], stage, 0, 0, outer)

    def radial_in(stage):
        return remote(u.at[stage, :, G : 2 * G], u.at[stage, :, G + nr : nr + 2 * G], stage, 1, 1, inner)

    def theta_copies(stage, late):
        up = jnp.where(last, 1, 0)
        down = jnp.where(first, 0, 1)
        src, dst = (tb, rb) if late else (ta, ra)
        base = 6 if late else 2
        return (
            remote(src.at[stage, 1, 8 - G : 8], dst.at[stage, up], stage, base, base + up, above),
            remote(src.at[stage, 0, 0:G], dst.at[stage, down], stage, base + 1, base + down, below),
        )

    def phi_copies(stage, late):
        src, dst, _, n, edge = sent[late]
        head, tail = pl.ds(0, edge), pl.ds(8 * n - edge, edge)
        base = 8 if late else 4
        return (
            remote(src.at[stage, 1, tail], dst.at[stage, 0, tail], stage, base, base, right),
            remote(src.at[stage, 0, head], dst.at[stage, 1, head], stage, base + 1, base + 1, left),
        )

    def send_early(stage):
        @pl.when(has_outer)
        def _():
            radial_out(stage).start()

        @pl.when(has_inner)
        def _():
            radial_in(stage).start()

        if not (isinstance(stage, int) and stage == 0):
            turn_early(stage)
        for c in phi_copies(stage, False) + theta_copies(stage, False):
            c.start()

    def send_late(stage):
        turn_late(stage)
        for c in phi_copies(stage, True) + theta_copies(stage, True):
            c.start()

    for c in loads:
        c.wait()

    def prepare_first(late):
        def part(q, carry):
            r = plane_of(q)
            tiles = [[u[0, c, r + G, 8 * t : 8 * t + 8] for t in range(halves)] for c in range(6)]
            prepare(0, q, r, tiles, late)
            return carry

        return part

    lax.fori_loop(0, early, prepare_first(False), 0)
    lax.fori_loop(early, nr, prepare_first(True), 0)
    turn_early(0)
    pl.semaphore_wait(barrier, 4 + jnp.where(has_outer, 1, 0) + jnp.where(has_inner, 1, 0))
    send_early(0)
    send_late(0)

    def radial_faces(which):
        def part(t, carry):
            rows = pl.ds(pl.multiple_of(8 * t, 8), 8)
            for l in range(6):
                at = lambda j: lambda i: vr[j, i, rows]
                parts = (at(l), at(l + 4), at(l + 8)) if l < 4 else (at(l + 8), None, None)
                for span in which:
                    for i, x in faces(*parts, span):
                        gr[l, i, rows] = x
            return carry

        lax.fori_loop(0, halves, part, 0)

    def polar_faces(lo, hi, which, also):
        def part(q, carry):
            late = lo == 2
            n = rest if late else early
            for j in range(3):
                v = (0 if late else (1 + (j < 2)) * q) + (j if j < 2 else 0)
                base = 14 * early if late else 0
                at = lambda m: lambda i: vt[pl.ds(i * pitch14 + base + 4 * n * m + 8 * v, 8), :]
                parts = (at(0), at(1), at(2)) if j < 2 else (at(3), None, None)
                out = (6 * early if late else 0) + (4 * n if j == 2 else 0) + 8 * v
                for span in which:
                    for i, x in faces(*parts, span):
                        gt[pl.ds(i * pitch6 + out, 8), :] = x
                if also is not None:
                    also(q, j)
            return carry

        lax.fori_loop(lo, hi, part, 0)

    def azimuth_faces(lo, hi, which):
        def part(q, carry):
            a, s = lane_a[q], lane_s[q]
            swapped = jnp.where(q == 0, 3, jnp.where(q == 1, 0, 9))

            def at(block, i):
                return tt[block, pl.ds(first_row + place(i - G), 8, stride=jump), :]

            own = [kept(lambda i, c=c: at(3 * q + c, i)) for c in range(3)]
            fluxes = (
                lambda i: s * own[2](i) - a * at(swapped + 1, i),
                lambda i: a * at(swapped, i),
                None,
            )
            for c in range(3):
                k = kept(lambda i: wave_speed * own[c](i))
                f = kept(fluxes[c]) if fluxes[c] else None
                parts = (lambda i: f(i) + k(i), lambda i: f(i) - k(i), f) if f else (k, None, None)
                for span in which:
                    before = None
                    for i, x in faces(*parts, span):
                        if span[0] == G and (i == G or i == seg - G):
                            ga[3 * q + c, int(i != G)] = x
                        if span[0] == i == seg - G + 1:
                            before = ga[3 * q + c, 1]
                        if before is not None:
                            dd[3 * q + c, pl.ds(i - 1, 8, stride=jump), :] = coef_phi * (x - before)
                        before = x
                    if span == range(0, G):
                        dd[3 * q + c, pl.ds(G - 1, 8, stride=jump), :] = coef_phi * (ga[3 * q + c, 0] - before)
            return carry

        lax.fori_loop(lo, hi, part, 0)

    def turn_back(q, j):
        b = 3 * q + j
        x = jnp.concatenate([dd[b, pl.ds(place(8 * i), 8), :] for i in range(L // 8)], axis=0).T
        acc[b] = x.reshape(full, nt, L)

    inside_r = (range(G, nr - G + 1),)
    edges_r = (range(0, G), range(nr - G + 1, nr + 1))
    inside_t = (range(G, nt - G + 1),)
    inside_a = (range(G, seg - G + 1),)
    edges_a = (range(0, G), range(seg - G + 1, seg + 1))
    edges_t = (range(0, G), range(nt - G + 1, nt + 1))

    def azimuth_ghosts(stage, late):
        for c in phi_copies(stage, late):
            c.wait_recv()
        before, after = first_row + place(-G) - (8 - G), first_row + place(L)
        _, dst, b0, n, _ = sent[late]
        for b in range(b0, b0 + n):
            x, y = (dst[stage, i, pl.ds(b - b0, 8, stride=n), :] for i in range(2))
            tt[b, pl.ds(before, 8), :] = x
            tt[b, pl.ds(after, 8), :] = y
            if 6 <= b < 8:
                tt[b + 3, pl.ds(before, 8), :] = pltpu.roll(x, L // 2, 1)
                tt[b + 3, pl.ds(after, 8), :] = pltpu.roll(y, L // 2, 1)

    def polar_ghosts(stage, late):
        src, dst, base = ((ta, ra, 2), (tb, rb, 6))[late]
        q0, n = groups[late]
        a, s = car[8 * late : 8 * late + n], csr[8 * late : 8 * late + n]
        for side in range(2):
            remote(src.at[stage, side, 0:G], dst.at[stage, side], stage, base, base + side, above).wait_recv()
            pole = first if side == 0 else last
            sign = jnp.where(pole, -1.0, 1.0)
            for g in range(G):
                k = jnp.where(pole, G - 1 - g, g)
                target = g if side == 0 else G + nt + g
                x = [dst[stage, side, k, c * n : c * n + n] for c in range(6)]
                x = [y * sign if c % 3 else y for c, y in enumerate(x)]
                for l, y in enumerate(lines(1, x, polar_flux(x, a, s))):
                    vt[pl.ds(target * pitch14 + spot(l, q0, late), n), :] = y

    def stage_body(stage, carry, ending=False):
        radial_faces(inside_r)
        polar_faces(0, 2, inside_t, None)
        azimuth_faces(0, 3, inside_a)
        polar_faces(2, 3, inside_t, None)

        azimuth_ghosts(stage, 0)
        azimuth_faces(0, 2, edges_a)
        @pl.when(has_inner)
        def _():
            radial_out(stage).wait_recv()

        @pl.when(has_outer)
        def _():
            radial_in(stage).wait_recv()

        def ghost_planes(q, carry):
            p = jnp.where(q < G, q, q + nr)
            a, s = ca[p], cs[p]
            for t in range(halves):
                rows = slice(8 * t, 8 * t + 8)
                x = [u[stage, c, p, rows] for c in range(6)]
                for l, y in enumerate(lines(0, x, radial_flux(x, a, s))):
                    vr[l, p, rows] = y
            return carry

        lax.fori_loop(0, 2 * G, ghost_planes, 0)
        radial_faces(edges_r)

        polar_ghosts(stage, 0)
        polar_faces(0, 2, edges_t, turn_back)

        w = jnp.where(stage == 0, 0.0, jnp.where(stage == 1, 0.75, 1.0 / 3.0)).astype(jnp.float32)

        def update(q, late):
            r = plane_of(q)
            rp, rm = crp[r + G], crm[r + G]
            new = [[None] * halves for _ in range(6)]
            for t in range(halves):
                rows = slice(8 * t, 8 * t + 8)
                for c in range(6):
                    lr, lt = AXES[0].index(c), AXES[1].index(c)
                    at = spot(lt, q, late, 6)
                    low = gt[pl.ds(8 * t * pitch6 + at, 8, stride=pitch6), :]
                    high = gt[pl.ds((8 * t + 1) * pitch6 + at, 8, stride=pitch6), :]
                    block, level = (6 + c % 3, q - early + rest * (c // 3)) if late else (c, q)
                    rate = acc[block, level, rows] + (cth[0, rows] * high - cth[1, rows] * low)
                    rate = rate + (rp * gr[lr, r + 1, rows] - rm * gr[lr, r, rows])
                    new[c][t] = w * u[0, c, r + G, rows] + (1.0 - w) * (u[stage, c, r + G, rows] + rate)
                b, d = [new[c][t] for c in range(3)], [new[c][t] for c in range(3, 6)]
                b2 = jnp.maximum(b[0] * b[0] + b[1] * b[1] + b[2] * b[2], 1.0)
                along = (b[0] * d[0] + b[1] * d[1] + b[2] * d[2]) * pl.reciprocal(b2, approx=True)
                d = [y - along * x for x, y in zip(b, d)]
                d2 = d[0] * d[0] + d[1] * d[1] + d[2] * d[2]
                shrink = b2 * lax.rsqrt(b2 * jnp.maximum(d2, b2))
                for c in range(3):
                    new[3 + c][t] = d[c] * shrink
            return new

        def keep(q, new, late):
            r = plane_of(q)
            for t in range(halves):
                rows = slice(8 * t, 8 * t + 8)
                for c in range(6):
                    if ending:
                        (mag_out, ele_out)[c // 3][c % 3, r, rows] = new[c][t]
                    else:
                        u[stage + 1, c, r + G, rows] = new[c][t]
            if not ending:
                prepare(stage + 1, q, r, new, late)

        def final(late, pair):
            def part(i, carry):
                new = [update(pair * i + j, late) for j in range(pair)]
                for j in range(pair):
                    keep(pair * i + j, new[j], late)
                return carry

            return part

        lax.fori_loop(0, early // 2, final(False, 2), 0)
        if not ending:
            send_early(stage + 1)
        azimuth_ghosts(stage, 1)
        azimuth_faces(2, 3, edges_a)
        polar_ghosts(stage, 1)
        polar_faces(2, 3, edges_t, turn_back)
        lax.fori_loop(early // 2, nr // 2, final(True, 2), 0)
        if not ending:
            send_late(stage + 1)
        return carry

    lax.fori_loop(0, 2, stage_body, 0)
    stage_body(2, 0, True)

    def drain(stage, carry):
        @pl.when(has_outer)
        def _():
            radial_out(stage).wait_send()

        @pl.when(has_inner)
        def _():
            radial_in(stage).wait_send()

        for c in theta_copies(stage, False) + theta_copies(stage, True) + phi_copies(stage, False) + phi_copies(stage, True):
            c.wait_send()
        return carry

    lax.fori_loop(0, 3, drain, 0)


def solution(mesh):
    n_row, n_theta, n_phi = (mesh.shape[k] for k in ("row", "theta", "phi"))

    def put_out(m, e, mo, eo, sem):
        copies = [pltpu.make_async_copy(x, y, sem.at[i]) for i, (x, y) in enumerate(((m, mo), (e, eo)))]
        for c in copies:
            c.start()
        for c in copies:
            c.wait()

    def body(magnetic, electric):
        _, nr, nt, lanes = magnetic.shape
        planes, rest = nr + 2 * G, nr - lanes // nt
        pad8 = lambda n: -(-n // 8) * 8
        f32 = jnp.float32
        vm = lambda *shape: pltpu.VMEM(shape, f32)
        assert nt % 8 == 0 and nr % 4 == 0 and 2 * nr * nt == 3 * lanes
        long = lanes + 8 * PAD
        sizes = (n_row, n_theta, n_phi, nr, nt, lanes)
        anywhere = pl.BlockSpec(memory_space=pl.ANY)
        out = pl.pallas_call(
            functools.partial(kernel, sizes),
            out_shape=[pltpu.VMEM(magnetic.shape, f32)] * 2,
            in_specs=[anywhere] * 2,
            out_specs=[pl.BlockSpec(memory_space=pltpu.VMEM)] * 2,
            scratch_shapes=[
                vm(3, 6, planes, nt, lanes),
                vm(3, 2, 8, 6 * 2 * rest, lanes),
                vm(3, 2, 8, 6 * rest, lanes),
                vm(3, 2, G, 6 * 2 * rest, lanes),
                vm(3, 2, G, 6 * rest, lanes),
                vm(3, 2, 8 * 6, lanes),
                vm(3, 2, 8 * 3, lanes),
                vm(3, 2, 8 * 6, lanes),
                vm(3, 2, 8 * 3, lanes),
                vm(11, 16 + pad8(long) + 8, lanes),
                vm(9, pad8(long), lanes),
                vm(14, planes, nt, lanes),
                vm(pad8((nt + 2 * G) * (14 * nr + PAD)), lanes),
                vm(6, nr + 1, nt, lanes),
                vm(pad8((nt + 1) * (6 * nr + PAD)), lanes),
                vm(9, 2, 8, lanes),
                vm(9, lanes // nt, nt, lanes),
                vm(planes, 8, lanes),
                vm(planes, 8, lanes),
                vm(16, lanes),
                vm(16, lanes),
                vm(planes, 8, lanes),
                vm(planes, 8, lanes),
                vm(2, nt, lanes),
                vm(3, 8, lanes),
                vm(3, 8, lanes),
                pltpu.SemaphoreType.DMA((3, 10)),
                pltpu.SemaphoreType.DMA((3, 10)),
                pltpu.SemaphoreType.DMA((2,)),
            ],
            compiler_params=pltpu.CompilerParams(
                collective_id=0, has_side_effects=True
            ),
        )(magnetic, electric)
        return pl.pallas_call(
            put_out,
            out_shape=[jax.ShapeDtypeStruct(magnetic.shape, f32)] * 2,
            in_specs=[pl.BlockSpec(memory_space=pltpu.VMEM)] * 2,
            out_specs=[anywhere] * 2,
            scratch_shapes=[pltpu.SemaphoreType.DMA((2,))],
            compiler_params=pltpu.CompilerParams(vmem_limit_bytes=4 * 2**20),
        )(*out)

    spec = P(None, "row", "theta", "phi")
    return jax.shard_map(body, mesh=mesh, in_specs=(spec, spec), out_specs=(spec, spec), check_vma=False)
```

```python
import functools
import math

import jax
import jax.numpy as jnp
from jax import lax
from jax.experimental import pallas as pl
from jax.experimental.pallas import tpu as pltpu
from jax.sharding import PartitionSpec as P

MESH = pl.DeviceIdType.MESH
hole_mass = 1.0
inner_radius = 1.8
wave_speed = 1.25
courant = 0.3
smooth_eps = 1e-06
G = 3

AXES = ((1, 2, 4, 5, 0, 3), (0, 2, 3, 5, 1, 4))
PAD = 1


def kept(make):
    made = {}

    def get(i):
        if i not in made:
            made[i] = make(i)
        return made[i]

    return get


class Line:
    def __init__(self, v):
        self.v = v
        self.d = kept(lambda i: v(i + 1) - v(i))
        self.e = kept(lambda i: self.d(i) * self.d(i) + 4.0 * smooth_eps)
        self.e4 = kept(lambda i: 4.0 * self.e(i))
        self.step = kept(lambda i: self.d(i) - self.d(i - 1))
        self.s2 = kept(lambda i: self.step(i) * self.step(i))
        self.t = kept(lambda i: self.step(i + 1) - self.step(i))
        self.t2 = kept(lambda i: 0.5 * self.t(i))
        self.sum = kept(lambda i: self.e(i - 1) + self.e(i))
        self.rest = kept(lambda i: (11.0 / 3.0) * self.s2(i) - self.sum(i))
        self.mid = kept(lambda i: self.sum(i) + (5.0 / 3.0) * self.s2(i))
        self.low = kept(lambda i: self.rest(i) + self.e4(i))
        self.high = kept(lambda i: self.rest(i) + self.e4(i - 1))
        self.w_low, self.w_mid, self.w_high = (
            kept(lambda i, x=x: self.weight(x(i))) for x in (self.low, self.mid, self.high)
        )
        self.mid6 = kept(lambda i: 6.0 * self.w_mid(i))

    def weight(self, smooth):
        q = pl.reciprocal(smooth, approx=True)
        return q * q

    def up(self, c):
        return ratio(self.low(c - 1), self.mid(c), self.high(c + 1), self.t(c - 1), self.t2(c))

    def down(self, c):
        return ratio(self.high(c + 2), self.mid(c + 1), self.low(c), self.t(c + 1), self.t2(c))

    def both(self, c):
        return blend(
            self.w_low(c - 1), self.mid6(c), 3.0 * self.w_high(c + 1), self.t(c - 1), self.t2(c)
        ) + blend(
            self.w_high(c + 2), self.mid6(c + 1), 3.0 * self.w_low(c), self.t(c + 1), self.t2(c)
        )


def blend(w0, w1, w2, t0, t2):
    den = (w0 + w2) + w1
    return (w0 * t0 + w2 * t2) * pl.reciprocal(den, approx=True)


def ratio(s0, s1, s2, t0, t2):
    y0, y2 = s1 * pl.reciprocal(s0, approx=True), s1 * pl.reciprocal(s2, approx=True)
    return blend(y0 * y0, 6.0, 3.0 * (y2 * y2), t0, t2)


def faces(p, m, f, which):
    line = Line(kept(p))
    if m is None:
        for i in which:
            c = i + 2
            yield i, line.t2(c) - line.both(c)
        return
    other = Line(kept(m))
    f = kept(f)
    f5, f2 = kept(lambda i: 5.0 * f(i)), kept(lambda i: f(i) + f(i))
    for i in which:
        c = i + 2
        lin = (f5(c) + (f2(c + 1) - f(c - 1))) - other.t2(c)
        yield i, lin - (line.up(c) - other.down(c))


def kernel(sizes, mag, ele, mag_out, ele_out, u, ta, tb, ra, rb, pa, pb, qa, qb, tt, dd, vr, vt, gr, gt, ga, acc,
           ca, cs, car, csr, crp, crm, cth, lane_a, lane_s, send, recv, local):
    n_row, n_theta, n_phi, nr, nt, L = sizes
    row, th, ph = lax.axis_index("row"), lax.axis_index("theta"), lax.axis_index("phi")
    halves = nt // 8
    spacing = math.pi / (nt * n_theta)
    spacing_phi = 2.0 * math.pi / (L * n_phi)
    dt = courant / (1.0 / spacing + 1.0 / spacing + 1.0 / spacing_phi)
    scale = -dt / 6.0
    coef_phi = scale / spacing_phi
    planes = nr + 2 * G
    rows6, rows14 = 6 * nr, 14 * nr
    pitch6, pitch14 = rows6 + PAD, rows14 + PAD
    full, rest = L // nt, nr - L // nt
    seg = L // 8
    jump = seg + PAD
    first_row = 16
    sent = ((pa, qa, 0, 6, 24), (pb, qb, 6, 3, 16))
    early = 2 * rest
    groups = ((0, early), (early, rest))
    ta_rows = ta.reshape(3, 2, 8 * 6 * early, L)
    tb_rows = tb.reshape(3, 2, 8 * 6 * rest, L)

    def spot(l, q, late, lines=14):
        return lines * early + l * rest + q - early if late else l * early + q

    def plane_of(q):
        return q + full if isinstance(q, int) and q < rest else (
            q - rest if isinstance(q, int) else jnp.where(q < rest, q + full, q - rest))

    def place(m):
        return m % seg + (m // seg) * jump

    first, last = th == 0, th == n_theta - 1
    opposite = (row, th, lax.rem(ph + n_phi // 2, n_phi))
    right = (row, th, lax.rem(ph + 1, n_phi))
    left = (row, th, lax.rem(ph + n_phi - 1, n_phi))
    above = tuple(jnp.where(last, o, q) for o, q in zip(opposite, (row, th + 1, ph)))
    below = tuple(jnp.where(first, o, q) for o, q in zip(opposite, (row, th - 1, ph)))
    outer, inner = (row + 1, th, ph), (row - 1, th, ph)
    has_outer, has_inner = row < n_row - 1, row > 0

    barrier = pltpu.get_barrier_semaphore()
    for target in (above, below, right, left):
        pl.semaphore_signal(barrier, inc=1, device_id=target, device_id_type=MESH)

    @pl.when(has_outer)
    def _():
        pl.semaphore_signal(barrier, inc=1, device_id=outer, device_id_type=MESH)

    @pl.when(has_inner)
    def _():
        pl.semaphore_signal(barrier, inc=1, device_id=inner, device_id_type=MESH)

    loads = [
        pltpu.make_async_copy(src, u.at[0, 3 * i : 3 * i + 3, G : G + nr], local.at[i])
        for i, src in enumerate((mag, ele))
    ]
    for c in loads:
        c.start()

    lane = lax.broadcasted_iota(jnp.int32, (8, L), 1)
    sub = lax.broadcasted_iota(jnp.int32, (8, L), 0)

    def radius_at(index):
        return inner_radius + (index.astype(jnp.float32) + 0.5) * spacing

    def lapse_shift(radius):
        ratio = 2.0 * hole_mass / radius
        return 1.0 / jnp.sqrt(1.0 + ratio), ratio / (1.0 + ratio)

    for i, (q0, _) in enumerate(groups):
        index = q0 + sub
        a, s = lapse_shift(radius_at(row * nr + jnp.where(index < rest, index + full, index - rest)))
        car[8 * i : 8 * i + 8] = a
        csr[8 * i : 8 * i + 8] = s

    def tables(q, carry):
        index = jnp.full((8, L), row * nr - G + q, jnp.int32)
        a, s = lapse_shift(radius_at(index))
        ca[q] = a
        cs[q] = s
        rc, hi, lo = radius_at(index), radius_at(index + 1), radius_at(index - 1)
        area = scale / (rc * rc * spacing)
        crp[q] = (0.5 * (rc + hi)) ** 2 * area
        crm[q] = (0.5 * (rc + lo)) ** 2 * area
        return carry

    lax.fori_loop(0, planes, tables, 0)
    for q in range(halves):
        index = (th * nt + 8 * q + sub).astype(jnp.float32)
        mid = jnp.sin((index + 0.5) * spacing)
        cth[0, 8 * q : 8 * q + 8] = scale * jnp.sin((index + 1.0) * spacing) / (mid * spacing)
        cth[1, 8 * q : 8 * q + 8] = scale * jnp.sin(index * spacing) / (mid * spacing)

    def owner(x, size):
        out = jnp.zeros((8, L), jnp.int32)
        for q in range(1, L // size):
            out = out + (x >= size * q).astype(jnp.int32)
        return out

    index = owner(lane, nt)
    a, s = lapse_shift(radius_at(row * nr + jnp.where(index < rest, index + full, index - rest)))
    lane_a[0], lane_a[1] = a, -a
    lane_s[0], lane_s[1] = s, s
    second = lane >= L // 2
    a, s = lapse_shift(radius_at(row * nr + rest + owner(jnp.where(second, lane - L // 2, lane), nt)))
    lane_a[2], lane_s[2] = jnp.where(second, -a, a), s

    zeros = jnp.zeros((nt, L), jnp.float32)
    for stage in range(3):
        @pl.when(row == 0)
        def _():
            for c in range(6):
                for q in range(G):
                    u[stage, c, q] = zeros

        @pl.when(row == n_row - 1)
        def _():
            for c in range(6):
                for q in range(G):
                    u[stage, c, G + nr + q] = zeros

    def radial_flux(x, a, s):
        b2, b3, d2, d3 = x[1], x[2], x[4], x[5]
        return [-(a * d3 + s * b2), a * d2 - s * b3, a * b3 - s * d2, -(a * b2 + s * d3)]

    def polar_flux(x, a, s):
        b1, b2, b3, d1, d2, d3 = x
        return [a * d3 + s * b2, -(a * d1), s * d2 - a * b3, a * b1]

    def lines(dim, x, f):
        k = [wave_speed * y for y in x]
        two = [k[c] for c in AXES[dim][:4]]
        return (
            [y + z for y, z in zip(f, two)] + [y - z for y, z in zip(f, two)] + f + [k[c] for c in AXES[dim][4:]]
        )

    def prepare(stage, q, r, tiles, late):
        a, s = ca[r + G], cs[r + G]
        for t in range(halves):
            rows = slice(8 * t, 8 * t + 8)
            x = [tiles[c][t] for c in range(6)]
            for l, y in enumerate(lines(0, x, radial_flux(x, a, s))):
                vr[l, r + G, rows] = y
            for l, y in enumerate(lines(1, x, polar_flux(x, a, s))):
                vt[pl.ds((G + 8 * t) * pitch14 + spot(l, q, late), 8, stride=pitch14), :] = y
            for side, end in enumerate((0, halves - 1)):
                if t == end:
                    for c in range(6):
                        if late:
                            tb_rows[stage, side, pl.ds(c * rest + q - early, 8, stride=6 * rest), :] = x[c]
                        else:
                            ta_rows[stage, side, pl.ds(c * early + q, 8, stride=6 * early), :] = x[c]

    def turn(stage, out, parts):
        x = jnp.concatenate([u[stage, c, G + p : G + p + n].reshape(n * nt, L) for c, p, n in parts], axis=0).T
        for q in range(L // 8):
            tt[out, pl.ds(first_row + place(8 * q), 8), :] = x[8 * q : 8 * q + 8]
        for src, _, b, n, _ in sent:
            if b <= out < b + n:
                src[stage, 0, pl.ds(out - b, 8, stride=n), :] = x[0:8]
                src[stage, 1, pl.ds(out - b, 8, stride=n), :] = x[L - 8 : L]

    def turn_early(stage):
        for c in range(6):
            turn(stage, c, [(c, full, rest), (c, 0, full - rest)])

    def turn_late(stage):
        p = full - rest
        for c in range(3):
            turn(stage, 6 + c, [(c, p, rest), (3 + c, p, rest)])
        for c in range(2):
            turn(stage, 9 + c, [(3 + c, p, rest), (c, p, rest)])

    def remote(src, dst, stage, m_send, m_recv, target):
        return pltpu.make_async_remote_copy(
            src_ref=src, dst_ref=dst, send_sem=send.at[stage, m_send], recv_sem=recv.at[stage, m_recv],
            device_id=target, device_id_type=MESH,
        )

    def radial_out(stage):
        return remote(u.at[stage, :, nr : nr + G], u.at[stage, :, 0:G], stage, 0, 0, outer)

    def radial_in(stage):
        return remote(u.at[stage, :, G : 2 * G], u.at[stage, :, G + nr : nr + 2 * G], stage, 1, 1, inner)

    def theta_copies(stage, late):
        up = jnp.where(last, 1, 0)
        down = jnp.where(first, 0, 1)
        src, dst = (tb, rb) if late else (ta, ra)
        base = 6 if late else 2
        return (
            remote(src.at[stage, 1, 8 - G : 8], dst.at[stage, up], stage, base, base + up, above),
            remote(src.at[stage, 0, 0:G], dst.at[stage, down], stage, base + 1, base + down, below),
        )

    def phi_copies(stage, late):
        src, dst, _, n, edge = sent[late]
        head, tail = pl.ds(0, edge), pl.ds(8 * n - edge, edge)
        base = 8 if late else 4
        return (
            remote(src.at[stage, 1, tail], dst.at[stage, 0, tail], stage, base, base, right),
            remote(src.at[stage, 0, head], dst.at[stage, 1, head], stage, base + 1, base + 1, left),
        )

    def send_early(stage):
        @pl.when(has_outer)
        def _():
            radial_out(stage).start()

        @pl.when(has_inner)
        def _():
            radial_in(stage).start()

        if not (isinstance(stage, int) and stage == 0):
            turn_early(stage)
        for c in phi_copies(stage, False) + theta_copies(stage, False):
            c.start()

    def send_late(stage):
        turn_late(stage)
        for c in phi_copies(stage, True) + theta_copies(stage, True):
            c.start()

    for c in loads:
        c.wait()

    def prepare_first(late):
        def part(q, carry):
            r = plane_of(q)
            tiles = [[u[0, c, r + G, 8 * t : 8 * t + 8] for t in range(halves)] for c in range(6)]
            prepare(0, q, r, tiles, late)
            return carry

        return part

    lax.fori_loop(0, early, prepare_first(False), 0)
    lax.fori_loop(early, nr, prepare_first(True), 0)
    turn_early(0)
    pl.semaphore_wait(barrier, 4 + jnp.where(has_outer, 1, 0) + jnp.where(has_inner, 1, 0))
    send_early(0)
    send_late(0)

    def radial_faces(which):
        def part(t, carry):
            rows = pl.ds(pl.multiple_of(8 * t, 8), 8)
            for l in range(6):
                at = lambda j: lambda i: vr[j, i, rows]
                parts = (at(l), at(l + 4), at(l + 8)) if l < 4 else (at(l + 8), None, None)
                for span in which:
                    for i, x in faces(*parts, span):
                        gr[l, i, rows] = x
            return carry

        lax.fori_loop(0, halves, part, 0)

    def polar_faces(lo, hi, which, also):
        def part(q, carry):
            late = lo == 2
            n = rest if late else early
            for j in range(3):
                v = (0 if late else (1 + (j < 2)) * q) + (j if j < 2 else 0)
                base = 14 * early if late else 0
                at = lambda m: lambda i: vt[pl.ds(i * pitch14 + base + 4 * n * m + 8 * v, 8), :]
                parts = (at(0), at(1), at(2)) if j < 2 else (at(3), None, None)
                out = (6 * early if late else 0) + (4 * n if j == 2 else 0) + 8 * v
                for span in which:
                    for i, x in faces(*parts, span):
                        gt[pl.ds(i * pitch6 + out, 8), :] = x
                if also is not None:
                    also(q, j)
            return carry

        lax.fori_loop(lo, hi, part, 0)

    def azimuth_faces(lo, hi, which):
        def part(q, carry):
            a, s = lane_a[q], lane_s[q]
            swapped = jnp.where(q == 0, 3, jnp.where(q == 1, 0, 9))

            def at(block, i):
                return tt[block, pl.ds(first_row + place(i - G), 8, stride=jump), :]

            own = [kept(lambda i, c=c: at(3 * q + c, i)) for c in range(3)]
            fluxes = (
                lambda i: s * own[2](i) - a * at(swapped + 1, i),
                lambda i: a * at(swapped, i),
                None,
            )
            for c in range(3):
                k = kept(lambda i: wave_speed * own[c](i))
                f = kept(fluxes[c]) if fluxes[c] else None
                parts = (lambda i: f(i) + k(i), lambda i: f(i) - k(i), f) if f else (k, None, None)
                for span in which:
                    before = None
                    for i, x in faces(*parts, span):
                        if span[0] == G and (i == G or i == seg - G):
                            ga[3 * q + c, int(i != G)] = x
                        if span[0] == i == seg - G + 1:
                            before = ga[3 * q + c, 1]
                        if before is not None:
                            dd[3 * q + c, pl.ds(i - 1, 8, stride=jump), :] = coef_phi * (x - before)
                        before = x
                    if span == range(0, G):
                        dd[3 * q + c, pl.ds(G - 1, 8, stride=jump), :] = coef_phi * (ga[3 * q + c, 0] - before)
            return carry

        lax.fori_loop(lo, hi, part, 0)

    def turn_back(q, j):
        b = 3 * q + j
        x = jnp.concatenate([dd[b, pl.ds(place(8 * i), 8), :] for i in range(L // 8)], axis=0).T
        acc[b] = x.reshape(full, nt, L)

    inside_r = (range(G, nr - G + 1),)
    edges_r = (range(0, G), range(nr - G + 1, nr + 1))
    inside_t = (range(G, nt - G + 1),)
    inside_a = (range(G, seg - G + 1),)
    edges_a = (range(0, G), range(seg - G + 1, seg + 1))
    edges_t = (range(0, G), range(nt - G + 1, nt + 1))

    def azimuth_ghosts(stage, late):
        for c in phi_copies(stage, late):
            c.wait_recv()
        before, after = first_row + place(-G) - (8 - G), first_row + place(L)
        _, dst, b0, n, _ = sent[late]
        for b in range(b0, b0 + n):
            x, y = (dst[stage, i, pl.ds(b - b0, 8, stride=n), :] for i in range(2))
            tt[b, pl.ds(before, 8), :] = x
            tt[b, pl.ds(after, 8), :] = y
            if 6 <= b < 8:
                tt[b + 3, pl.ds(before, 8), :] = pltpu.roll(x, L // 2, 1)
                tt[b + 3, pl.ds(after, 8), :] = pltpu.roll(y, L // 2, 1)

    def polar_ghosts(stage, late):
        src, dst, base = ((ta, ra, 2), (tb, rb, 6))[late]
        q0, n = groups[late]
        a, s = car[8 * late : 8 * late + n], csr[8 * late : 8 * late + n]
        for side in range(2):
            remote(src.at[stage, side, 0:G], dst.at[stage, side], stage, base, base + side, above).wait_recv()
            pole = first if side == 0 else last
            sign = jnp.where(pole, -1.0, 1.0)
            for g in range(G):
                k = jnp.where(pole, G - 1 - g, g)
                target = g if side == 0 else G + nt + g
                x = [dst[stage, side, k, c * n : c * n + n] for c in range(6)]
                x = [y * sign if c % 3 else y for c, y in enumerate(x)]
                for l, y in enumerate(lines(1, x, polar_flux(x, a, s))):
                    vt[pl.ds(target * pitch14 + spot(l, q0, late), n), :] = y

    def stage_body(stage, carry, ending=False):
        radial_faces(inside_r)
        polar_faces(0, 2, inside_t, None)
        azimuth_faces(0, 3, inside_a)
        polar_faces(2, 3, inside_t, None)

        azimuth_ghosts(stage, 0)
        azimuth_faces(0, 2, edges_a)
        @pl.when(has_inner)
        def _():
            radial_out(stage).wait_recv()

        @pl.when(has_outer)
        def _():
            radial_in(stage).wait_recv()

        def ghost_planes(q, carry):
            p = jnp.where(q < G, q, q + nr)
            a, s = ca[p], cs[p]
            for t in range(halves):
                rows = slice(8 * t, 8 * t + 8)
                x = [u[stage, c, p, rows] for c in range(6)]
                for l, y in enumerate(lines(0, x, radial_flux(x, a, s))):
                    vr[l, p, rows] = y
            return carry

        lax.fori_loop(0, 2 * G, ghost_planes, 0)
        radial_faces(edges_r)

        polar_ghosts(stage, 0)
        polar_faces(0, 2, edges_t, turn_back)

        w = jnp.where(stage == 0, 0.0, jnp.where(stage == 1, 0.75, 1.0 / 3.0)).astype(jnp.float32)

        def update(q, late):
            r = plane_of(q)
            rp, rm = crp[r + G], crm[r + G]
            new = [[None] * halves for _ in range(6)]
            for t in range(halves):
                rows = slice(8 * t, 8 * t + 8)
                for c in range(6):
                    lr, lt = AXES[0].index(c), AXES[1].index(c)
                    at = spot(lt, q, late, 6)
                    low = gt[pl.ds(8 * t * pitch6 + at, 8, stride=pitch6), :]
                    high = gt[pl.ds((8 * t + 1) * pitch6 + at, 8, stride=pitch6), :]
                    block, level = (6 + c % 3, q - early + rest * (c // 3)) if late else (c, q)
                    rate = acc[block, level, rows] + (cth[0, rows] * high - cth[1, rows] * low)
                    rate = rate + (rp * gr[lr, r + 1, rows] - rm * gr[lr, r, rows])
                    new[c][t] = w * u[0, c, r + G, rows] + (1.0 - w) * (u[stage, c, r + G, rows] + rate)
                b, d = [new[c][t] for c in range(3)], [new[c][t] for c in range(3, 6)]
                b2 = jnp.maximum(b[0] * b[0] + b[1] * b[1] + b[2] * b[2], 1.0)
                along = (b[0] * d[0] + b[1] * d[1] + b[2] * d[2]) * pl.reciprocal(b2, approx=True)
                d = [y - along * x for x, y in zip(b, d)]
                d2 = d[0] * d[0] + d[1] * d[1] + d[2] * d[2]
                shrink = b2 * lax.rsqrt(b2 * jnp.maximum(d2, b2))
                for c in range(3):
                    new[3 + c][t] = d[c] * shrink
            return new

        def keep(q, new, late):
            r = plane_of(q)
            for t in range(halves):
                rows = slice(8 * t, 8 * t + 8)
                for c in range(6):
                    if ending:
                        (mag_out, ele_out)[c // 3][c % 3, r, rows] = new[c][t]
                    else:
                        u[stage + 1, c, r + G, rows] = new[c][t]
            if not ending:
                prepare(stage + 1, q, r, new, late)

        def final(late, pair):
            def part(i, carry):
                new = [update(pair * i + j, late) for j in range(pair)]
                for j in range(pair):
                    keep(pair * i + j, new[j], late)
                return carry

            return part

        lax.fori_loop(0, early // 2, final(False, 2), 0)
        if not ending:
            send_early(stage + 1)
        azimuth_ghosts(stage, 1)
        azimuth_faces(2, 3, edges_a)
        polar_ghosts(stage, 1)
        polar_faces(2, 3, edges_t, turn_back)
        lax.fori_loop(early // 2, nr // 2, final(True, 2), 0)
        if not ending:
            send_late(stage + 1)
        return carry

    lax.fori_loop(0, 2, stage_body, 0)
    stage_body(2, 0, True)

    def drain(stage, carry):
        @pl.when(has_outer)
        def _():
            radial_out(stage).wait_send()

        @pl.when(has_inner)
        def _():
            radial_in(stage).wait_send()

        for c in theta_copies(stage, False) + theta_copies(stage, True) + phi_copies(stage, False) + phi_copies(stage, True):
            c.wait_send()
        return carry

    lax.fori_loop(0, 3, drain, 0)


def solution(mesh):
    n_row, n_theta, n_phi = (mesh.shape[k] for k in ("row", "theta", "phi"))

    def put_out(m, e, mo, eo, sem):
        copies = [pltpu.make_async_copy(x, y, sem.at[i]) for i, (x, y) in enumerate(((m, mo), (e, eo)))]
        for c in copies:
            c.start()
        for c in copies:
            c.wait()

    def body(magnetic, electric):
        _, nr, nt, lanes = magnetic.shape
        planes, rest = nr + 2 * G, nr - lanes // nt
        pad8 = lambda n: -(-n // 8) * 8
        f32 = jnp.float32
        vm = lambda *shape: pltpu.VMEM(shape, f32)
        assert nt % 8 == 0 and nr % 4 == 0 and 2 * nr * nt == 3 * lanes
        long = lanes + 8 * PAD
        sizes = (n_row, n_theta, n_phi, nr, nt, lanes)
        anywhere = pl.BlockSpec(memory_space=pl.ANY)
        out = pl.pallas_call(
            functools.partial(kernel, sizes),
            out_shape=[pltpu.VMEM(magnetic.shape, f32)] * 2,
            in_specs=[anywhere] * 2,
            out_specs=[pl.BlockSpec(memory_space=pltpu.VMEM)] * 2,
            scratch_shapes=[
                vm(3, 6, planes, nt, lanes),
                vm(3, 2, 8, 6 * 2 * rest, lanes),
                vm(3, 2, 8, 6 * rest, lanes),
                vm(3, 2, G, 6 * 2 * rest, lanes),
                vm(3, 2, G, 6 * rest, lanes),
                vm(3, 2, 8 * 6, lanes),
                vm(3, 2, 8 * 3, lanes),
                vm(3, 2, 8 * 6, lanes),
                vm(3, 2, 8 * 3, lanes),
                vm(11, 16 + pad8(long) + 8, lanes),
                vm(9, pad8(long), lanes),
                vm(14, planes, nt, lanes),
                vm(pad8((nt + 2 * G) * (14 * nr + PAD)), lanes),
                vm(6, nr + 1, nt, lanes),
                vm(pad8((nt + 1) * (6 * nr + PAD)), lanes),
                vm(9, 2, 8, lanes),
                vm(9, lanes // nt, nt, lanes),
                vm(planes, 8, lanes),
                vm(planes, 8, lanes),
                vm(16, lanes),
                vm(16, lanes),
                vm(planes, 8, lanes),
                vm(planes, 8, lanes),
                vm(2, nt, lanes),
                vm(3, 8, lanes),
                vm(3, 8, lanes),
                pltpu.SemaphoreType.DMA((3, 10)),
                pltpu.SemaphoreType.DMA((3, 10)),
                pltpu.SemaphoreType.DMA((2,)),
            ],
            compiler_params=pltpu.CompilerParams(
                collective_id=0, has_side_effects=True
            ),
        )(magnetic, electric)
        return pl.pallas_call(
            put_out,
            out_shape=[jax.ShapeDtypeStruct(magnetic.shape, f32)] * 2,
            in_specs=[pl.BlockSpec(memory_space=pltpu.VMEM)] * 2,
            out_specs=[anywhere] * 2,
            scratch_shapes=[pltpu.SemaphoreType.DMA((2,))],
            compiler_params=pltpu.CompilerParams(vmem_limit_bytes=4 * 2**20),
        )(*out)

    spec = P(None, "row", "theta", "phi")
    return jax.shard_map(body, mesh=mesh, in_specs=(spec, spec), out_specs=(spec, spec), check_vma=False)
```
